16 devices in a mesh: batch: 2 (over y, z), seq: 8 (over x, core).
Axes of the slice: x: 4, y: 2, z: 1, core: 2. Of those that a mesh axis runs over, the one named last changes fastest.
The devices are a block of a 4x4x8 slice.
Arguments:
- hidden: bfloat16 [32, 4, 7168], P('batch'), parts along dimension 0
- cache_lens: int32 [32], P('batch'), parts along dimension 0
- c_kv: bfloat16 [32, 16384, 512], P('batch', 'seq'), parts along dimension 0
- k_r: bfloat16 [32, 16384, 64], P('batch', 'seq'), parts along dimension 0
- w_uq: bfloat16 [7168, 128, 128], P(None, 'seq')
- w_qr: bfloat16 [7168, 128, 64], P(None, 'seq')
- w_uk: bfloat16 [128, 128, 512], P('seq')
- w_uv: bfloat16 [128, 512, 128], P('seq')
- w_o: bfloat16 [128, 128, 7168], P('seq')
Outputs:
- output: bfloat16 [32, 4, 7168], P('batch'), parts along dimension 0
There are 2 independent parts. The reference program is written for one: setup_inputs(seed, part) draws one part's arguments, and reference() takes and returns one part's arrays. A program takes and returns all parts, laid end to end along the dimension named above; an argument that names none is the same for every part.
All inputs are finite; a program needn't handle non-finite values.
Results may differ from the reference program's by a relative error of at most 0.00666237.
Values are sent between devices in bfloat16 or wider.
A program may use at most 768 MiB of HBM per device.

```python
import jax
import jax.numpy as jnp
from jax import lax

ROW_COUNT = 16
CTX_LEN = 16384
Q_LEN = 4
MODEL_DIM = 7168
NUM_HEADS = 128
NOPE_DIM = 128
ROPE_DIM = 64
LATENT_DIM = 512
VALUE_DIM = 128


def setup_inputs(seed: int = 0, part: int = 0) -> dict:
    part_key = jax.random.fold_in(jax.random.key(seed), part)
    key_x, key_lens, key_cache, key_rope = jax.random.split(part_key, 4)
    key_uq, key_qr, key_uk, key_uv, key_wo = jax.random.split(jax.random.key(seed + 1), 5)
    hidden = jax.random.normal(key_x, (ROW_COUNT, Q_LEN, MODEL_DIM), jnp.float32)
    short_by = jax.random.randint(key_lens, (ROW_COUNT,), 0, CTX_LEN // 4 + 1)
    cache_lens = (CTX_LEN - Q_LEN - short_by).at[0].set(CTX_LEN - Q_LEN)
    c_kv = jax.random.normal(key_cache, (ROW_COUNT, CTX_LEN, LATENT_DIM), jnp.float32)
    k_r = jax.random.normal(key_rope, (ROW_COUNT, CTX_LEN, ROPE_DIM), jnp.float32)
    w_uq = jax.random.normal(key_uq, (MODEL_DIM, NUM_HEADS, NOPE_DIM), jnp.float32) * MODEL_DIM ** -0.5
    w_qr = jax.random.normal(key_qr, (MODEL_DIM, NUM_HEADS, ROPE_DIM), jnp.float32) * (2.0 * MODEL_DIM ** -0.5)
    w_uk = jax.random.normal(key_uk, (NUM_HEADS, NOPE_DIM, LATENT_DIM), jnp.float32) * (2.0 * NOPE_DIM ** -0.5)
    w_uv = jax.random.normal(key_uv, (NUM_HEADS, LATENT_DIM, VALUE_DIM), jnp.float32) * LATENT_DIM ** -0.5
    w_o = jax.random.normal(key_wo, (NUM_HEADS, VALUE_DIM, MODEL_DIM), jnp.float32) * (2.0 * (NUM_HEADS * VALUE_DIM) ** -0.5)
    return {
        "hidden": hidden.astype(jnp.bfloat16),
        "cache_lens": cache_lens.astype(jnp.int32),
        "c_kv": c_kv.astype(jnp.bfloat16),
        "k_r": k_r.astype(jnp.bfloat16),
        "w_uq": w_uq.astype(jnp.bfloat16),
        "w_qr": w_qr.astype(jnp.bfloat16),
        "w_uk": w_uk.astype(jnp.bfloat16),
        "w_uv": w_uv.astype(jnp.bfloat16),
        "w_o": w_o.astype(jnp.bfloat16),
    }


def reference(hidden, cache_lens, c_kv, k_r, w_uq, w_qr, w_uk, w_uv, w_o):
    hidden_wide = hidden.astype(jnp.float32)
    q_nope = jnp.einsum("bqd,dhk->bqhk", hidden_wide, w_uq.astype(jnp.float32)).astype(jnp.bfloat16)
    q_rope = jnp.einsum("bqd,dhr->bqhr", hidden_wide, w_qr.astype(jnp.float32)).astype(jnp.bfloat16)
    q_lat = jnp.einsum("bqhk,hkc->bqhc", q_nope.astype(jnp.float32), w_uk.astype(jnp.float32)).astype(jnp.bfloat16)
    score_scale = (NOPE_DIM + ROPE_DIM) ** -0.5
    positions = jnp.arange(CTX_LEN)
    offsets = jnp.arange(Q_LEN)

    def row_attend(row_args):
        lat_row, rope_row, cache_row, key_row, row_len = row_args
        cache_wide = cache_row.astype(jnp.float32)
        scores = (jnp.einsum("qhc,tc->qht", lat_row.astype(jnp.float32), cache_wide)
                  + jnp.einsum("qhr,tr->qht", rope_row.astype(jnp.float32), key_row.astype(jnp.float32))) * score_scale
        visible = positions[None, None, :] <= (row_len + offsets)[:, None, None]
        probs = jax.nn.softmax(jnp.where(visible, scores, -jnp.inf), axis=-1)
        return jnp.einsum("qht,tc->qhc", probs, cache_wide)

    o_lat = lax.map(row_attend, (q_lat, q_rope, c_kv, k_r, cache_lens)).astype(jnp.bfloat16)
    o_val = jnp.einsum("bqhc,hcv->bqhv", o_lat.astype(jnp.float32), w_uv.astype(jnp.float32)).astype(jnp.bfloat16)
    y_sum = jnp.einsum("bqhv,hvd->bqd", o_val.astype(jnp.float32), w_o.astype(jnp.float32))
    return (hidden_wide + y_sum).astype(jnp.bfloat16)
```

```python
import functools

import jax
import jax.numpy as jnp
from jax import lax
from jax.experimental import pallas as pl
from jax.experimental.pallas import tpu as pltpu
from jax.sharding import PartitionSpec as P

MASK_FILL = -1e30
LOG2E = 1.4426950408889634
MESH = pl.DeviceIdType.MESH
LAG_B, LAG_C, LAG_D = 1, 3, 5
PIECES = 4


def remote(src, dst, send_sem, recv_sem, dev):
    return pltpu.make_async_remote_copy(src_ref=src, dst_ref=dst, send_sem=send_sem, recv_sem=recv_sem,
                                        device_id={"seq": dev}, device_id_type=MESH)


def place(chips):
    me = lax.axis_index("seq")
    x, c = me // 2, lax.rem(me, 2)
    xr, xl = lax.rem(x + 1, chips), lax.rem(x + chips - 1, chips)
    return x, c, xr, xl, 2 * xr + c, 2 * xl + c, 2 * x + 1 - c


def greet(devs):
    barrier = pltpu.get_barrier_semaphore()
    for dev in devs:
        pl.semaphore_signal(barrier, inc=1, device_id={"seq": dev}, device_id_type=MESH)
    pl.semaphore_wait(barrier, len(devs))


def gather_kernel(chips, lat_ref, rope_ref, lat_all, rope_all, send, recv, local):
    x, c, xr, xl, right, left, partner = place(chips)
    xo = lax.rem(x + 2, chips)
    step = lat_ref.shape[0] // PIECES
    pairs = ((lat_ref, lat_all), (rope_ref, rope_all))
    half = PIECES // 2
    greet((right, left, partner))
    rows = lambda p: pl.ds(p * step, step)

    def copy(a, p, kind, src, slot, dev):
        return remote(src, pairs[a][1].at[rows(p), slot[1], slot[0]], send.at[a, p, kind], recv.at[a, p, kind], dev)

    def own(a, p, kind, dev):
        return copy(a, p, kind, pairs[a][0].at[rows(p)], (x, c), dev)

    def pass_on(a, p, kind, block, dev):
        return copy(a, p, kind, pairs[a][1].at[rows(p), c, block], (block, c), dev)

    def landed(a, p, kind, block, core):
        ref = pairs[a][1].at[rows(p), core, block]
        return remote(ref, ref, send.at[a, p, kind], recv.at[a, p, kind], partner)

    keep = lambda a: pltpu.make_async_copy(pairs[a][0], pairs[a][1].at[:, c, x], local.at[a])
    order_l = [(p + half) % PIECES for p in range(PIECES)]
    for i in range(PIECES):
        for a in range(2):
            own(a, i, 0, right).start()
            own(a, order_l[i], 1, left).start()
    for p in range(PIECES):
        for a in range(2):
            own(a, p, 2, partner).start()
    for a in range(2):
        keep(a).start()
    for i in range(PIECES):
        for a in range(2):
            landed(a, i, 0, xl, c).wait_recv()
            if i < half:
                pass_on(a, i, 3, xl, right).start()
            pass_on(a, i, 4, xl, partner).start()
            p = order_l[i]
            landed(a, p, 1, xr, c).wait_recv()
            if p >= half:
                pass_on(a, p, 3, xr, left).start()
            pass_on(a, p, 5, xr, partner).start()
    for p in range(PIECES):
        for a in range(2):
            landed(a, p, 3, xo, c).wait_recv()
            pass_on(a, p, 6, xo, partner).start()
    for p in range(PIECES):
        for a in range(2):
            for kind, block in ((2, x), (4, xl), (5, xr), (6, xo)):
                landed(a, p, kind, block, 1 - c).wait_recv()
            own(a, p, 0, right).wait_send()
            own(a, p, 1, left).wait_send()
            own(a, p, 2, partner).wait_send()
            if p < half:
                pass_on(a, p, 3, xl, right).wait_send()
            else:
                pass_on(a, p, 3, xr, left).wait_send()
            pass_on(a, p, 4, xl, partner).wait_send()
            pass_on(a, p, 5, xr, partner).wait_send()
            pass_on(a, p, 6, xo, partner).wait_send()
    for a in range(2):
        keep(a).wait()


def gather(chips, lat, rope):
    rows = lat.shape[0]
    return pl.pallas_call(
        functools.partial(gather_kernel, chips),
        out_shape=[jax.ShapeDtypeStruct((rows, 2, chips) + lat.shape[1:], lat.dtype),
                   jax.ShapeDtypeStruct((rows, 2, chips) + rope.shape[1:], rope.dtype)],
        in_specs=[pl.BlockSpec(memory_space=pltpu.VMEM)] * 2,
        out_specs=[pl.BlockSpec(memory_space=pl.ANY)] * 2,
        scratch_shapes=[pltpu.SemaphoreType.DMA((2, PIECES, 7)), pltpu.SemaphoreType.DMA((2, PIECES, 7)),
                        pltpu.SemaphoreType.DMA((2,))],
        compiler_params=pltpu.CompilerParams(collective_id=0, has_side_effects=True),
        name="gather_queries",
    )(lat, rope)


def expand(ml):
    col = jnp.transpose(jnp.broadcast_to(ml[0:1, :], (128, 128)))
    return col[0:64, :], col[64:128, :]


def compact(m, l):
    return jnp.transpose(jnp.concatenate([m, l], axis=0))[0:8, :]


def attend_kernel(chips, rows, scale, lens_ref, lat_ref, rope_ref, ckv_ref, kr_ref, out_ref,
                  s_buf, p_buf, away_o, away_ml, home_o, home_ml, d2d_o, d2d_ml, one_o, one_ml, two_o, two_ml,
                  send, recv):
    x, c, xr, xl, right, left, partner = place(chips)
    xo = lax.rem(x + 2, chips)
    i = pl.program_id(0)
    local_len = ckv_ref.shape[1]
    width = ckv_ref.shape[2]
    nq = lat_ref.shape[2]
    gq = nq // chips
    hq = gq // 2
    heads = gq // 4
    k2 = scale * LOG2E
    lanes = [pl.ds(j * 128, 128) for j in range(width // 128)]

    def moves(r):
        return (
            (away_o.at[r], d2d_o.at[r], partner),
            (away_ml.at[r], d2d_ml.at[r], partner),
            (home_o.at[r, xo, pl.ds(0, hq)], one_o.at[r, 0], right),
            (home_ml.at[r, xo], one_ml.at[r, 0], right),
            (home_o.at[r, xo, pl.ds(hq, hq)], one_o.at[r, 1], left),
            (home_ml.at[r, xo], one_ml.at[r, 1], left),
            (home_o.at[r, xr], two_o.at[r, 0], right),
            (home_ml.at[r, xr], two_ml.at[r, 0], right),
            (home_o.at[r, xl], two_o.at[r, 1], left),
            (home_ml.at[r, xl], two_ml.at[r, 1], left),
        )

    def copy(r, kind):
        src, dst, dev = moves(r)[kind]
        return remote(src, dst, send.at[r, kind], recv.at[r, kind], dev)

    @pl.when(i == 0)
    def _():
        greet((right, left, partner))

    @pl.when(i < rows)
    def _():
        base = (2 * x + c) * local_len
        seen = lens_ref[jnp.minimum(i, rows - 1)] - base
        col = lax.broadcasted_iota(jnp.int32, (nq, local_len), 1)
        tok = lax.rem(lax.broadcasted_iota(jnp.int32, (nq, local_len), 0), gq) // heads
        visible = col - tok <= seen
        contract = (((1,), (1,)), ((), ()))

        def scores(n, block):
            packed = rope_ref[0, block]
            part = packed.shape[0] // chips
            rope = jnp.concatenate(
                [packed[g * part:(g + 1) * part, h * 64:(h + 1) * 64] for g in range(chips) for h in range(2)], axis=0)
            s = lax.dot_general(lat_ref[0, block], ckv_ref[0], contract, preferred_element_type=jnp.float32)
            s = s + jnp.dot(rope, kr_ref[0], preferred_element_type=jnp.float32)
            s_buf[n] = jnp.where(visible, s, MASK_FILL)

        def weigh(n):
            s = s_buf[n]
            m = jnp.max(s, axis=1, keepdims=True)
            p = jnp.exp2((s - m) * k2)
            l = jnp.sum(p, axis=1, keepdims=True)
            p_buf[n] = p.astype(jnp.bfloat16)
            return m, l

        def mix(n, m, l, o_ref, ml_ref):
            o = jnp.dot(p_buf[n], ckv_ref[0], preferred_element_type=jnp.float32)
            m = jnp.broadcast_to(m, (nq, 128))
            l = jnp.broadcast_to(l, (nq, 128))
            for g in range(chips):
                at = slice(g * gq, (g + 1) * gq)
                o_ref[i, g] = o[at]
                ml_ref[i, g] = compact(m[at], l[at])

        scores(0, 1 - c)
        scores(1, c)
        ml0 = weigh(0)
        mix(0, *ml0, away_o, away_ml)
        copy(i, 0).start()
        copy(i, 1).start()
        ml1 = weigh(1)
        mix(1, *ml1, home_o, home_ml)

    @pl.when((i >= LAG_B) & (i < rows + LAG_B))
    def _():
        r = i - LAG_B
        copy(r, 0).wait_recv()
        copy(r, 1).wait_recv()
        for g in range(chips):
            ma, la = expand(home_ml[r, g])
            mb, lb = expand(d2d_ml[r, g])
            m = jnp.maximum(ma, mb)
            fa, fb = jnp.exp2((ma - m) * k2), jnp.exp2((mb - m) * k2)
            for at in lanes:
                home_o[r, g, :, at] = home_o[r, g, :, at] * fa + d2d_o[r, g, :, at] * fb
            home_ml[r, g] = compact(m, la * fa + lb * fb)
        for kind in range(2, 6):
            copy(r, kind).start()

    @pl.when((i >= LAG_C) & (i < rows + LAG_C))
    def _():
        r = i - LAG_C
        for kind in range(2, 6):
            copy(r, kind).wait_recv()
        for side, g in ((0, xr), (1, xl)):
            part = slice(side * hq, (side + 1) * hq)
            ma, la = expand(home_ml[r, g])
            mb, lb = expand(one_ml[r, side])
            m = jnp.maximum(ma, mb)[part]
            fa, fb = jnp.exp2((ma[part] - m) * k2), jnp.exp2((mb[part] - m) * k2)
            for at in lanes:
                home_o[r, g, pl.ds(side * hq, hq), at] = (home_o[r, g, pl.ds(side * hq, hq), at] * fa
                                                          + one_o[r, side, :, at] * fb)
            l = la[part] * fa + lb[part] * fb
            if side == 0:
                m, l = jnp.concatenate([m, ma[hq:]], axis=0), jnp.concatenate([l, la[hq:]], axis=0)
            else:
                m, l = jnp.concatenate([ma[:hq], m], axis=0), jnp.concatenate([la[:hq], l], axis=0)
            home_ml[r, g] = compact(m, l)
        for kind in range(6, 10):
            copy(r, kind).start()

    @pl.when(i >= LAG_D)
    def _():
        r = i - LAG_D
        for kind in range(6, 10):
            copy(r, kind).wait_recv()
        ma, la = expand(home_ml[r, x])
        mb, lb = expand(two_ml[r, 0])
        mc, lc = expand(two_ml[r, 1])
        m = jnp.maximum(ma, jnp.maximum(mb, mc))
        fa, fb, fc = jnp.exp2((ma - m) * k2), jnp.exp2((mb - m) * k2), jnp.exp2((mc - m) * k2)
        l = la * fa + lb * fb + lc * fc
        for at in lanes:
            o = home_o[r, x, :, at] * fa + two_o[r, 0, :, at] * fb + two_o[r, 1, :, at] * fc
            out_ref[0, :, at] = (o / l).astype(out_ref.dtype)

    @pl.when(i == rows + LAG_D - 1)
    def _():
        @pl.loop(0, rows)
        def _(r):
            for kind in range(10):
                copy(r, kind).wait_send()


def attend(chips, scale, lens, lat, rope, ckv, kr):
    rows, _, nq, width = lat.shape
    gq = nq // chips
    local_len = ckv.shape[1]
    row = lambda i: jnp.minimum(i, rows - 1)
    f32, bf16 = jnp.float32, jnp.bfloat16
    return pl.pallas_call(
        functools.partial(attend_kernel, chips, rows, scale),
        grid=(rows + LAG_D,),
        out_shape=jax.ShapeDtypeStruct((rows, gq, width), bf16),
        in_specs=[pl.BlockSpec(memory_space=pltpu.SMEM),
                  pl.BlockSpec((1,) + lat.shape[1:], lambda i: (row(i), 0, 0, 0)),
                  pl.BlockSpec((1,) + rope.shape[1:], lambda i: (row(i), 0, 0, 0)),
                  pl.BlockSpec((1,) + ckv.shape[1:], lambda i: (row(i), 0, 0)),
                  pl.BlockSpec((1,) + kr.shape[1:], lambda i: (row(i), 0, 0))],
        out_specs=pl.BlockSpec((1, gq, width), lambda i: (jnp.maximum(i - LAG_D, 0), 0, 0)),
        scratch_shapes=[
            pltpu.VMEM((2, nq, local_len), f32), pltpu.VMEM((2, nq, local_len), bf16),
            pltpu.VMEM((rows, chips, gq, width), f32), pltpu.VMEM((rows, chips, 8, 128), f32),
            pltpu.VMEM((rows, chips, gq, width), f32), pltpu.VMEM((rows, chips, 8, 128), f32),
            pltpu.VMEM((rows, chips, gq, width), f32), pltpu.VMEM((rows, chips, 8, 128), f32),
            pltpu.VMEM((rows, 2, gq // 2, width), f32), pltpu.VMEM((rows, 2, 8, 128), f32),
            pltpu.VMEM((rows, 2, gq, width), f32), pltpu.VMEM((rows, 2, 8, 128), f32),
            pltpu.SemaphoreType.DMA((rows, 10)), pltpu.SemaphoreType.DMA((rows, 10))],
        compiler_params=pltpu.CompilerParams(collective_id=1, has_side_effects=True,
                                             dimension_semantics=("arbitrary",), vmem_limit_bytes=67_000_000),
        name="attend_merge",
    )(lens, lat, rope, ckv, kr)


def output_kernel(chips, ov_ref, hid_ref, w_ref, out_ref, w_buf, away, near, home, far,
                  w_sem, send, recv):
    x, c, xr, xl, right, left, partner = place(chips)
    me = 2 * x + c
    xo = lax.rem(x + 2, chips)
    cols = w_buf.shape[2]
    span = lambda dev: pl.ds(pl.multiple_of(dev * cols, 128), cols)
    dests = (xo, xr, xl, x)

    def load(k, first):
        core = 1 - c if first else c
        n = 2 * k + (0 if first else 1)
        return pltpu.make_async_copy(w_ref.at[:, span(2 * dests[k] + core)], w_buf.at[n], w_sem.at[n])

    for k in range(chips):
        load(k, True).start()
        load(k, False).start()
    peers = tuple(2 * d + c for d in dests[:3])
    greet(peers + (partner,))

    def swap(k):
        return remote(away.at[k], near.at[k], send.at[0, k], recv.at[0, k], partner)

    def reduce(k):
        return remote(home.at[k], far.at[k], send.at[1, k], recv.at[1, k], peers[k])

    for k in range(chips):
        load(k, True).wait()
        away[k] = jnp.dot(ov_ref[...], w_buf[2 * k], preferred_element_type=jnp.float32)
        swap(k).start()
        load(k, False).wait()
        home[k] = jnp.dot(ov_ref[...], w_buf[2 * k + 1], preferred_element_type=jnp.float32)
        swap(k).wait_recv()
        home[k] = home[k] + near[k]
        if k < chips - 1:
            reduce(k).start()
    for k in range(chips - 1):
        reduce(k).wait_recv()
    y = home[chips - 1] + far[0] + far[1] + far[2]
    out_ref[:, span(me)] = (hid_ref[...].astype(jnp.float32) + y).astype(out_ref.dtype)

    def spread(k):
        return remote(out_ref.at[:, span(me)], out_ref.at[:, span(me)], send.at[2, k], recv.at[2, k], peers[k])

    def mirror(k):
        ref = out_ref.at[:, span(2 * dests[k] + c)]
        return remote(ref, ref, send.at[3, k], recv.at[3, k], partner)

    def landed(kind, k, dev):
        ref = out_ref.at[:, span(dev)]
        return remote(ref, ref, send.at[kind, k], recv.at[kind, k], partner)

    for k in range(chips - 1):
        spread(k).start()
    mirror(3).start()
    source = (xo, xl, xr)
    slot = (0, 2, 1)
    for k in (1, 2, 0):
        landed(2, k, 2 * source[k] + c).wait_recv()
        mirror(slot[k]).start()
    for k in range(chips):
        landed(3, k, 2 * ((xo, xr, xl, x)[k]) + 1 - c).wait_recv()
    for k in range(chips):
        swap(k).wait_send()
        mirror(k).wait_send()
        if k < chips - 1:
            reduce(k).wait_send()
            spread(k).wait_send()


def output(chips, o_val, hidden, w_o):
    tokens, depth = o_val.shape
    dim = w_o.shape[1]
    cols = dim // (2 * chips)
    f32 = jnp.float32
    vmem = pl.BlockSpec(memory_space=pltpu.VMEM)
    return pl.pallas_call(
        functools.partial(output_kernel, chips),
        out_shape=jax.ShapeDtypeStruct((tokens, dim), hidden.dtype),
        in_specs=[vmem, vmem, pl.BlockSpec(memory_space=pl.ANY)],
        out_specs=vmem,
        scratch_shapes=[
            pltpu.VMEM((2 * chips, depth, cols), w_o.dtype),
            pltpu.VMEM((chips, tokens, cols), f32), pltpu.VMEM((chips, tokens, cols), f32),
            pltpu.VMEM((chips, tokens, cols), f32), pltpu.VMEM((chips - 1, tokens, cols), f32),
            pltpu.SemaphoreType.DMA((2 * chips,)),
            pltpu.SemaphoreType.DMA((4, chips)), pltpu.SemaphoreType.DMA((4, chips))],
        compiler_params=pltpu.CompilerParams(collective_id=2, has_side_effects=True, vmem_limit_bytes=60_000_000),
        name="project_output",
    )(o_val, hidden, w_o)


def solution(mesh):
    chips = mesh.shape["seq"] // 2

    def local_step(hidden, cache_lens, c_kv, k_r, w_uq, w_qr, w_uk, w_uv, w_o):
        rows, toks, dim = hidden.shape
        heads, nope, width = w_uk.shape
        rope_dim = w_qr.shape[2]
        value = w_uv.shape[2]
        score_scale = (nope + rope_dim) ** -0.5
        f32, bf16 = jnp.float32, jnp.bfloat16
        q_nope = jnp.einsum("cre,eil->cril", hidden, w_uq, preferred_element_type=f32).astype(bf16)
        q_rope = jnp.einsum("cre,eis->cris", hidden, w_qr, preferred_element_type=f32).astype(bf16)
        q_lat = jnp.einsum("bqhk,hkc->bqhc", q_nope, w_uk, preferred_element_type=f32).astype(bf16)
        gq = toks * heads
        packed = q_rope.reshape(rows, 2, gq // 2, rope_dim).transpose(0, 2, 1, 3).reshape(rows, gq // 2, 2 * rope_dim)
        lat_all, rope_all = gather(chips, q_lat.reshape(rows, gq, width), packed)
        o_lat = attend(chips, score_scale, cache_lens,
                       lat_all.reshape(rows, 2, chips * gq, width),
                       rope_all.reshape(rows, 2, chips * gq // 2, 2 * rope_dim), c_kv, jnp.swapaxes(k_r, 1, 2))
        o_val = jnp.einsum("bqhc,hcv->bqhv", o_lat.reshape(rows, toks, heads, width), w_uv,
                           preferred_element_type=f32).astype(bf16)
        cols = dim // (2 * chips)
        own = lax.dynamic_slice_in_dim(hidden, lax.axis_index("seq") * cols, cols, axis=2)
        out = output(chips, o_val.reshape(rows * toks, heads * value), own.reshape(rows * toks, cols),
                     w_o.reshape(heads * value, dim))
        return out.reshape(rows, toks, dim)

    specs_in = (P("batch", None, None), P("batch"), P("batch", "seq", None), P("batch", "seq", None),
                P(None, "seq", None), P(None, "seq", None), P("seq", None, None), P("seq", None, None),
                P("seq", None, None))
    return jax.shard_map(local_step, mesh=mesh, in_specs=specs_in, out_specs=P("batch", None, None), check_vma=False)
```

```python
import functools

import jax
import jax.numpy as jnp
from jax import lax
from jax.experimental import pallas as pl
from jax.experimental.pallas import tpu as pltpu
from jax.sharding import PartitionSpec as P

MASK_FILL = -1e30
LOG2E = 1.4426950408889634
MESH = pl.DeviceIdType.MESH
LAG_B, LAG_C, LAG_D = 2, 4, 7
CUTS = 4


def remote(src, dst, send_sem, recv_sem, dev):
    return pltpu.make_async_remote_copy(src_ref=src, dst_ref=dst, send_sem=send_sem, recv_sem=recv_sem,
                                        device_id={"seq": dev}, device_id_type=MESH)


def place(chips):
    me = lax.axis_index("seq")
    x, c = me // 2, lax.rem(me, 2)
    xr, xl = lax.rem(x + 1, chips), lax.rem(x + chips - 1, chips)
    return x, c, xr, xl, 2 * xr + c, 2 * xl + c, 2 * x + 1 - c


def greet(devs):
    barrier = pltpu.get_barrier_semaphore()
    for dev in devs:
        pl.semaphore_signal(barrier, inc=1, device_id={"seq": dev}, device_id_type=MESH)
    pl.semaphore_wait(barrier, len(devs))


def pack(vals, dst, slot):
    n = vals[0].shape[0]
    low = lax.rem(lax.broadcasted_iota(jnp.int32, vals[0].shape, 0), 8) < 4
    even = [jnp.where(low, p, pltpu.roll(q, 4, 0)) for p, q in (vals[:2], vals[2:])]
    odd = [jnp.where(low, pltpu.roll(p, n - 4, 0), q) for p, q in (vals[:2], vals[2:])]
    for v in range(n // 8):
        at = slice(8 * v, 8 * v + 8)
        for side, both in ((0, even), (1, odd)):
            dst[2 * v + side, pl.ds(slot, 16)] = jnp.concatenate([both[0][at], both[1][at]], axis=0).astype(dst.dtype)


def query_kernel(chips, hid_ref, wq_ref, wr_ref, wk_ref, lat_all, rope_all,
                 wq_buf, wr_buf, wk_buf, wide, acc, lat_own, rope_own, wq_sem, wr_sem, wk_sem, send, recv, local):
    x, c, xr, xl, right, left, partner = place(chips)
    xo = lax.rem(x + 2, chips)
    rows, toks, dim = hid_ref.shape
    pairs, nope = wq_ref.shape[1], wq_ref.shape[3]
    per_ch = pairs // 2
    depth = dim // CUTS
    f32, bf16 = jnp.float32, jnp.bfloat16

    barrier = pltpu.get_barrier_semaphore()
    for dev in (right, left, partner):
        pl.semaphore_signal(barrier, inc=1, device_id={"seq": dev}, device_id_type=MESH)

    def load(u, k):
        return pltpu.make_async_copy(wq_ref.at[pl.ds(k * depth, depth), u], wq_buf.at[u, pl.ds(k * depth, depth)],
                                     wq_sem.at[u, k])

    def load_rope(k):
        n = wr_ref.shape[0] // CUTS
        return pltpu.make_async_copy(wr_ref.at[pl.ds(k * n, n)], wr_buf.at[pl.ds(k * n, n)], wr_sem.at[k])

    load_up = pltpu.make_async_copy(wk_ref, wk_buf, wk_sem)
    for k in range(CUTS):
        for u in range(per_ch):
            load(u, k).start()
    load_up.start()

    lane = lax.broadcasted_iota(jnp.int32, (128, 512), 1)
    src = lax.broadcasted_iota(jnp.int32, (128, 512), 0)
    spread = jnp.where(lax.rem(lane, 256) == 2 * src + lane // 256, 1.0, 0.0).astype(bf16)
    tiles = depth // 128
    n = rows * toks
    for k in range(CUTS):
        stack = jnp.concatenate([hid_ref[:, :, (k * tiles + t) * 128:(k * tiles + t + 1) * 128].reshape(n, 128)
                                 for t in range(tiles)], axis=0)
        res = jnp.dot(stack, spread, preferred_element_type=f32).astype(bf16)
        for t in range(tiles):
            for side in range(2):
                wide[k, pl.ds(side * n, n), pl.ds(t * 256, 256)] = res[t * n:(t + 1) * n, side * 256:side * 256 + 256]

    where = lambda p: pl.ds((p % 2) * 2 * 16 + (p // 2) * 16, 16) if p < 4 else pl.ds((p - 4) * 16, 16)
    own_ref = lambda p: (lat_own if p < 4 else rope_own).at[:, where(p)]
    all_ref = lambda p, core, block: (lat_all if p < 4 else rope_all).at[:, core, block, where(p)]

    def own(p, kind, dev):
        return remote(own_ref(p), all_ref(p, c, x), send.at[p, kind], recv.at[p, kind], dev)

    def pass_on(p, kind, block, dev):
        return remote(all_ref(p, c, block), all_ref(p, c, block), send.at[p, kind], recv.at[p, kind], dev)

    def landed(p, kind, block, core):
        ref = all_ref(p, core, block)
        return remote(ref, ref, send.at[p, kind], recv.at[p, kind], partner)

    keep = lambda p: pltpu.make_async_copy(own_ref(p), all_ref(p, c, x), local.at[p])

    def send_own(p):
        own(p, 0, right).start()
        own(p + 1, 0, right).start()
        own(p + 1, 1, left).start()
        own(p, 1, left).start()
        for q in (p, p + 1):
            own(q, 2, partner).start()
            keep(q).start()

    def relay(p):
        landed(p, 0, xl, c).wait_recv()
        pass_on(p, 3, xl, right).start()
        pass_on(p, 4, xl, partner).start()
        landed(p + 1, 1, xr, c).wait_recv()
        pass_on(p + 1, 3, xr, left).start()
        pass_on(p + 1, 5, xr, partner).start()
        landed(p + 1, 0, xl, c).wait_recv()
        pass_on(p + 1, 4, xl, partner).start()
        landed(p, 1, xr, c).wait_recv()
        pass_on(p, 5, xr, partner).start()

    for ch in range(2):
        base = ch * per_ch
        acc[...] = jnp.zeros_like(acc)

        @pl.loop(0, CUTS)
        def _(k):
            for u in range(base, base + per_ch):
                load(u, k).wait()
            if ch == 0:
                for u in range(per_ch, pairs):
                    load(u, k).start()
            else:
                load_rope(k).start()
            for j in range(per_ch // 2):
                w = [wq_buf[base + 2 * j + h, pl.ds(k * depth, depth)].reshape(2 * depth, nope) for h in range(2)]
                acc[j] += jnp.dot(wide[k], jnp.concatenate(w, axis=1), preferred_element_type=f32)

        if ch == 0:
            load_up.wait()
        for side in range(2):
            q_lat = []
            for u in range(per_ch):
                q_n = acc[u // 2, pl.ds(side * n, n), pl.ds((u % 2) * nope, nope)].astype(bf16)
                q_lat.append(jnp.dot(q_n, wk_buf[2 * (base + u) + side], preferred_element_type=f32))
            pack(q_lat, lat_own, side * 32 + ch * 16)
        if ch == 0:
            pl.semaphore_wait(barrier, 3)
        send_own(2 * ch)
    relay(0)

    tokens = jnp.concatenate([hid_ref[:, :, t * 128:(t + 1) * 128].reshape(n, 128) for t in range(dim // 128)], axis=1)
    part = wr_buf.shape[0] // CUTS
    q_rope = []
    for k in range(CUTS):
        load_rope(k).wait()
        r = lax.dot_general(tokens, wr_buf[pl.ds(k * part, part)], (((1,), (1,)), ((), ())), preferred_element_type=f32)
        q_rope += [r[:, j * 128:(j + 1) * 128] for j in range(part // 128)]
    for h in range(2):
        pack(q_rope[4 * h:4 * h + 4], rope_own, 16 * h)
    send_own(4)
    relay(2)
    relay(4)
    for p in range(6):
        landed(p, 3, xo, c).wait_recv()
        pass_on(p, 6, xo, partner).start()
    for p in range(6):
        for kind, block in ((2, x), (4, xl), (5, xr), (6, xo)):
            landed(p, kind, block, 1 - c).wait_recv()
        own(p, 0, right).wait_send()
        own(p, 1, left).wait_send()
        own(p, 2, partner).wait_send()
        if p % 2 == 0:
            pass_on(p, 3, xl, right).wait_send()
        else:
            pass_on(p, 3, xr, left).wait_send()
        pass_on(p, 4, xl, partner).wait_send()
        pass_on(p, 5, xr, partner).wait_send()
        pass_on(p, 6, xo, partner).wait_send()
        keep(p).wait()


def queries(chips, hidden, w_uq, w_qr, w_uk):
    rows, toks, dim = hidden.shape
    heads, nope, width = w_uk.shape
    gq = heads * toks
    bf16 = jnp.bfloat16
    wq = w_uq.reshape(dim, heads // 2, 2, nope)
    wr = jnp.transpose(w_qr, (1, 2, 0)).reshape(-1, dim)
    hbm = pl.BlockSpec(memory_space=pl.ANY)
    dma = pltpu.SemaphoreType.DMA
    return pl.pallas_call(
        functools.partial(query_kernel, chips),
        out_shape=[jax.ShapeDtypeStruct((rows, 2, chips, gq, width), bf16),
                   jax.ShapeDtypeStruct((rows, 2, chips, gq // 2, 128), bf16)],
        in_specs=[pl.BlockSpec(memory_space=pltpu.VMEM), hbm, hbm, hbm],
        out_specs=[hbm] * 2,
        scratch_shapes=[
            pltpu.VMEM((heads // 2, dim, 2, nope), bf16), pltpu.VMEM(wr.shape, bf16), pltpu.VMEM(w_uk.shape, bf16),
            pltpu.VMEM((CUTS, 2 * rows * toks, 2 * dim // CUTS), bf16),
            pltpu.VMEM((heads // 8, 2 * rows * toks, 2 * nope), jnp.float32),
            pltpu.VMEM((rows, gq, width), bf16), pltpu.VMEM((rows, gq // 2, 128), bf16),
            dma((heads // 2, CUTS)), dma((CUTS,)), dma(()), dma((6, 7)), dma((6, 7)), dma((6,))],
        compiler_params=pltpu.CompilerParams(collective_id=0, has_side_effects=True, vmem_limit_bytes=67_000_000),
        name="make_queries",
    )(hidden, wq, wr, w_uk)


def token(row):
    return lax.rem(row, 4)


def expand(ml):
    col = jnp.transpose(jnp.broadcast_to(ml[0:1, :], (128, 128)))
    return col[0:64, :], col[64:128, :]


def compact(m, l):
    return jnp.transpose(jnp.concatenate([m, l], axis=0))[0:8, :]


def attend_kernel(chips, rows, scale, lens_ref, lat_ref, rope_ref, ckv_ref, kr_ref, out_ref,
                  s_buf, p_buf, away_o, away_ml, home_o, home_ml, d2d_o, d2d_ml, one_o, one_ml, two_o, two_ml,
                  send, recv):
    x, c, xr, xl, right, left, partner = place(chips)
    xo = lax.rem(x + 2, chips)
    i = pl.program_id(0)
    local_len = ckv_ref.shape[1]
    width = ckv_ref.shape[2]
    nq = lat_ref.shape[2]
    gq = nq // chips
    hq = gq // 2
    k2 = scale * LOG2E
    lanes = [pl.ds(j * 128, 128) for j in range(width // 128)]

    def moves(r):
        return (
            (away_o.at[r], d2d_o.at[r], partner),
            (away_ml.at[r], d2d_ml.at[r], partner),
            (home_o.at[r, xo, pl.ds(0, hq)], one_o.at[r, 0], right),
            (home_ml.at[r, xo], one_ml.at[r, 0], right),
            (home_o.at[r, xo, pl.ds(hq, hq)], one_o.at[r, 1], left),
            (home_ml.at[r, xo], one_ml.at[r, 1], left),
            (home_o.at[r, xr], two_o.at[r, 0], right),
            (home_ml.at[r, xr], two_ml.at[r, 0], right),
            (home_o.at[r, xl], two_o.at[r, 1], left),
            (home_ml.at[r, xl], two_ml.at[r, 1], left),
        )

    def copy(r, kind):
        src, dst, dev = moves(r)[kind]
        return remote(src, dst, send.at[r, kind], recv.at[r, kind], dev)

    @pl.when(i == 0)
    def _():
        greet((right, left, partner))

    def late(lag):
        return jnp.where((i >= lag) & (i < rows + lag), i - lag, rows)

    def on_row(lag, act, kinds):
        @pl.when((i >= lag) & (i < rows + lag))
        def _():
            for kind in kinds:
                act(copy(i - lag, kind))

    def merge_pair():
        r = late(LAG_B)
        for g in range(chips):
            ma, la = expand(home_ml[r, g])
            mb, lb = expand(d2d_ml[r, g])
            m = jnp.maximum(ma, mb)
            fa, fb = jnp.exp2((ma - m) * k2), jnp.exp2((mb - m) * k2)
            for at in lanes:
                home_o[r, g, :, at] = home_o[r, g, :, at] * fa + d2d_o[r, g, :, at] * fb
            home_ml[r, g] = compact(m, la * fa + lb * fb)

    def merge_half():
        r = late(LAG_C)
        for side, g in ((0, xr), (1, xl)):
            part = slice(side * hq, (side + 1) * hq)
            ma, la = expand(home_ml[r, g])
            mb, lb = expand(one_ml[r, side])
            m = jnp.maximum(ma, mb)[part]
            fa, fb = jnp.exp2((ma[part] - m) * k2), jnp.exp2((mb[part] - m) * k2)
            for at in lanes:
                home_o[r, g, pl.ds(side * hq, hq), at] = (home_o[r, g, pl.ds(side * hq, hq), at] * fa
                                                          + one_o[r, side, :, at] * fb)
            l = la[part] * fa + lb[part] * fb
            if side == 0:
                m, l = jnp.concatenate([m, ma[hq:]], axis=0), jnp.concatenate([l, la[hq:]], axis=0)
            else:
                m, l = jnp.concatenate([ma[:hq], m], axis=0), jnp.concatenate([la[:hq], l], axis=0)
            home_ml[r, g] = compact(m, l)

    def finish():
        r = late(LAG_D)
        ma, la = expand(home_ml[r, x])
        mb, lb = expand(two_ml[r, 0])
        mc, lc = expand(two_ml[r, 1])
        m = jnp.maximum(ma, jnp.maximum(mb, mc))
        fa, fb, fc = jnp.exp2((ma - m) * k2), jnp.exp2((mb - m) * k2), jnp.exp2((mc - m) * k2)
        l = la * fa + lb * fb + lc * fc
        for at in lanes:
            o = home_o[r, x, :, at] * fa + two_o[r, 0, :, at] * fb + two_o[r, 1, :, at] * fc
            out_ref[0, :, at] = (o / l).astype(out_ref.dtype)

    on_row(LAG_B, lambda cp: cp.wait_recv(), range(0, 2))
    on_row(LAG_C, lambda cp: cp.wait_recv(), range(2, 6))
    on_row(LAG_D, lambda cp: cp.wait_recv(), range(6, 10))

    @pl.when(i < rows)
    def _():
        base = (2 * x + c) * local_len
        seen = lens_ref[jnp.minimum(i, rows - 1)] - base
        col = lax.broadcasted_iota(jnp.int32, (nq, local_len), 1)
        tok = token(lax.broadcasted_iota(jnp.int32, (nq, 1), 0))
        visible = col <= seen + tok
        contract = (((1,), (1,)), ((), ()))

        def scores(n, block):
            packed = rope_ref[0, block]
            part = packed.shape[0] // chips
            rope = jnp.concatenate(
                [packed[g * part:(g + 1) * part, h * 64:(h + 1) * 64] for g in range(chips) for h in range(2)], axis=0)
            s = lax.dot_general(lat_ref[0, block], ckv_ref[0], contract, preferred_element_type=jnp.float32)
            s = s + jnp.dot(rope, kr_ref[0], preferred_element_type=jnp.float32)
            s_buf[n] = jnp.where(visible, s, MASK_FILL)

        def weigh(n):
            s = s_buf[n]
            m = jnp.max(s, axis=1, keepdims=True)
            p = jnp.exp2((s - m) * k2)
            l = jnp.sum(p, axis=1, keepdims=True)
            p_buf[n] = p.astype(jnp.bfloat16)
            return m, l

        def mix(n, m, l, o_ref, ml_ref):
            o = jnp.dot(p_buf[n], ckv_ref[0], preferred_element_type=jnp.float32)
            m = jnp.broadcast_to(m, (nq, 128))
            l = jnp.broadcast_to(l, (nq, 128))
            for g in range(chips):
                at = slice(g * gq, (g + 1) * gq)
                o_ref[i, g] = o[at]
                ml_ref[i, g] = compact(m[at], l[at])

        merge_pair()
        scores(0, 1 - c)
        merge_half()
        scores(1, c)
        finish()
        ml0 = weigh(0)
        mix(0, *ml0, away_o, away_ml)
        ml1 = weigh(1)
        mix(1, *ml1, home_o, home_ml)

    @pl.when(i >= rows)
    def _():
        merge_pair()
        merge_half()
        finish()

    on_row(0, lambda cp: cp.start(), range(0, 2))
    on_row(LAG_B, lambda cp: cp.start(), range(2, 6))
    on_row(LAG_C, lambda cp: cp.start(), range(6, 10))

    @pl.when(i == rows + LAG_D - 1)
    def _():
        @pl.loop(0, rows)
        def _(r):
            for kind in range(10):
                copy(r, kind).wait_send()


def attend(chips, scale, lens, lat, rope, ckv, kr):
    rows, _, nq, width = lat.shape
    gq = nq // chips
    local_len = ckv.shape[1]
    row = lambda i: jnp.minimum(i, rows - 1)
    f32, bf16 = jnp.float32, jnp.bfloat16
    return pl.pallas_call(
        functools.partial(attend_kernel, chips, rows, scale),
        grid=(rows + LAG_D,),
        out_shape=jax.ShapeDtypeStruct((rows, gq, width), bf16),
        in_specs=[pl.BlockSpec(memory_space=pltpu.SMEM),
                  pl.BlockSpec((1,) + lat.shape[1:], lambda i: (row(i), 0, 0, 0)),
                  pl.BlockSpec((1,) + rope.shape[1:], lambda i: (row(i), 0, 0, 0)),
                  pl.BlockSpec((1,) + ckv.shape[1:], lambda i: (row(i), 0, 0)),
                  pl.BlockSpec((1,) + kr.shape[1:], lambda i: (row(i), 0, 0))],
        out_specs=pl.BlockSpec((1, gq, width), lambda i: (jnp.maximum(i - LAG_D, 0), 0, 0)),
        scratch_shapes=[
            pltpu.VMEM((2, nq, local_len), f32), pltpu.VMEM((2, nq, local_len), bf16),
            pltpu.VMEM((rows + 1, chips, gq, width), f32), pltpu.VMEM((rows + 1, chips, 8, 128), f32),
            pltpu.VMEM((rows + 1, chips, gq, width), f32), pltpu.VMEM((rows + 1, chips, 8, 128), f32),
            pltpu.VMEM((rows + 1, chips, gq, width), f32), pltpu.VMEM((rows + 1, chips, 8, 128), f32),
            pltpu.VMEM((rows + 1, 2, gq // 2, width), f32), pltpu.VMEM((rows + 1, 2, 8, 128), f32),
            pltpu.VMEM((rows + 1, 2, gq, width), f32), pltpu.VMEM((rows + 1, 2, 8, 128), f32),
            pltpu.SemaphoreType.DMA((rows, 10)), pltpu.SemaphoreType.DMA((rows, 10))],
        compiler_params=pltpu.CompilerParams(collective_id=1, has_side_effects=True,
                                             dimension_semantics=("arbitrary",), vmem_limit_bytes=67_000_000),
        name="attend_merge",
    )(lens, lat, rope, ckv, kr)


def output_kernel(chips, ov_ref, hid_ref, w_ref, out_ref, w_buf, away, near, home, far,
                  w_sem, send, recv):
    x, c, xr, xl, right, left, partner = place(chips)
    me = 2 * x + c
    xo = lax.rem(x + 2, chips)
    cols = w_buf.shape[2]
    span = lambda dev: pl.ds(pl.multiple_of(dev * cols, 128), cols)
    dests = (xo, xr, xl, x)

    def load(k, first):
        core = 1 - c if first else c
        n = 2 * k + (0 if first else 1)
        return pltpu.make_async_copy(w_ref.at[:, span(2 * dests[k] + core)], w_buf.at[n], w_sem.at[n])

    for k in range(chips):
        load(k, True).start()
        load(k, False).start()
    peers = tuple(2 * d + c for d in dests[:3])
    greet(peers + (partner,))

    def swap(k):
        return remote(away.at[k], near.at[k], send.at[0, k], recv.at[0, k], partner)

    def reduce(k):
        return remote(home.at[k], far.at[k], send.at[1, k], recv.at[1, k], peers[k])

    for k in range(chips):
        load(k, True).wait()
        away[k] = jnp.dot(ov_ref[...], w_buf[2 * k], preferred_element_type=jnp.float32)
        swap(k).start()
        load(k, False).wait()
        home[k] = jnp.dot(ov_ref[...], w_buf[2 * k + 1], preferred_element_type=jnp.float32)
        swap(k).wait_recv()
        home[k] = home[k] + near[k]
        if k < chips - 1:
            reduce(k).start()
    for k in range(chips - 1):
        reduce(k).wait_recv()
    y = home[chips - 1] + far[0] + far[1] + far[2]
    out_ref[:, span(me)] = (hid_ref[...].astype(jnp.float32) + y).astype(out_ref.dtype)

    def spread(k):
        return remote(out_ref.at[:, span(me)], out_ref.at[:, span(me)], send.at[2, k], recv.at[2, k], peers[k])

    def mirror(k):
        ref = out_ref.at[:, span(2 * dests[k] + c)]
        return remote(ref, ref, send.at[3, k], recv.at[3, k], partner)

    def landed(kind, k, dev):
        ref = out_ref.at[:, span(dev)]
        return remote(ref, ref, send.at[kind, k], recv.at[kind, k], partner)

    for k in range(chips - 1):
        spread(k).start()
    mirror(3).start()
    source = (xo, xl, xr)
    slot = (0, 2, 1)
    for k in (1, 2, 0):
        landed(2, k, 2 * source[k] + c).wait_recv()
        mirror(slot[k]).start()
    for k in range(chips):
        landed(3, k, 2 * ((xo, xr, xl, x)[k]) + 1 - c).wait_recv()
    for k in range(chips):
        swap(k).wait_send()
        mirror(k).wait_send()
        if k < chips - 1:
            reduce(k).wait_send()
            spread(k).wait_send()


def output(chips, o_val, hidden, w_o):
    tokens, depth = o_val.shape
    dim = w_o.shape[1]
    cols = dim // (2 * chips)
    f32 = jnp.float32
    vmem = pl.BlockSpec(memory_space=pltpu.VMEM)
    return pl.pallas_call(
        functools.partial(output_kernel, chips),
        out_shape=jax.ShapeDtypeStruct((tokens, dim), hidden.dtype),
        in_specs=[vmem, vmem, pl.BlockSpec(memory_space=pl.ANY)],
        out_specs=vmem,
        scratch_shapes=[
            pltpu.VMEM((2 * chips, depth, cols), w_o.dtype),
            pltpu.VMEM((chips, tokens, cols), f32), pltpu.VMEM((chips, tokens, cols), f32),
            pltpu.VMEM((chips, tokens, cols), f32), pltpu.VMEM((chips - 1, tokens, cols), f32),
            pltpu.SemaphoreType.DMA((2 * chips,)),
            pltpu.SemaphoreType.DMA((4, chips)), pltpu.SemaphoreType.DMA((4, chips))],
        compiler_params=pltpu.CompilerParams(collective_id=2, has_side_effects=True, vmem_limit_bytes=60_000_000),
        name="project_output",
    )(o_val, hidden, w_o)


def solution(mesh):
    chips = mesh.shape["seq"] // 2

    def local_step(hidden, cache_lens, c_kv, k_r, w_uq, w_qr, w_uk, w_uv, w_o):
        rows, toks, dim = hidden.shape
        heads, nope, width = w_uk.shape
        rope_dim = w_qr.shape[2]
        value = w_uv.shape[2]
        score_scale = (nope + rope_dim) ** -0.5
        f32, bf16 = jnp.float32, jnp.bfloat16
        gq = toks * heads
        lat_all, rope_all = queries(chips, hidden, w_uq, w_qr, w_uk)
        o_lat = attend(chips, score_scale, cache_lens,
                       lat_all.reshape(rows, 2, chips * gq, width),
                       rope_all.reshape(rows, 2, chips * gq // 2, 2 * rope_dim), c_kv, jnp.swapaxes(k_r, 1, 2))
        o_val = jnp.einsum("bpuqc,upcv->bqupv", o_lat.reshape(rows, 2, heads // 2, toks, width),
                           w_uv.reshape(heads // 2, 2, width, value), preferred_element_type=f32).astype(bf16)
        cols = dim // (2 * chips)
        own = lax.dynamic_slice_in_dim(hidden, lax.axis_index("seq") * cols, cols, axis=2)
        out = output(chips, o_val.reshape(rows * toks, heads * value), own.reshape(rows * toks, cols),
                     w_o.reshape(heads * value, dim))
        return out.reshape(rows, toks, dim)

    specs_in = (P("batch", None, None), P("batch"), P("batch", "seq", None), P("batch", "seq", None),
                P(None, "seq", None), P(None, "seq", None), P("seq", None, None), P("seq", None, None),
                P("seq", None, None))
    return jax.shard_map(local_step, mesh=mesh, in_specs=specs_in, out_specs=P("batch", None, None), check_vma=False)
```

```python
import functools

import jax
import jax.numpy as jnp
from jax import lax
from jax.experimental import pallas as pl
from jax.experimental.pallas import tpu as pltpu
from jax.sharding import PartitionSpec as P

MASK_FILL = -1e30
LOG2E = 1.4426950408889634
MESH = pl.DeviceIdType.MESH
LAG_B, LAG_C, LAG_D = 1, 3, 6
CUTS = 4
AHEAD = 3


def remote(src, dst, send_sem, recv_sem, dev):
    return pltpu.make_async_remote_copy(src_ref=src, dst_ref=dst, send_sem=send_sem, recv_sem=recv_sem,
                                        device_id={"seq": dev}, device_id_type=MESH)


def place(chips):
    me = lax.axis_index("seq")
    x, c = me // 2, lax.rem(me, 2)
    xr, xl = lax.rem(x + 1, chips), lax.rem(x + chips - 1, chips)
    return x, c, xr, xl, 2 * xr + c, 2 * xl + c, 2 * x + 1 - c


def greet(devs):
    barrier = pltpu.get_barrier_semaphore()
    for dev in devs:
        pl.semaphore_signal(barrier, inc=1, device_id={"seq": dev}, device_id_type=MESH)
    pl.semaphore_wait(barrier, len(devs))


def pack(vals, dst, slot):
    n = vals[0].shape[0]
    low = lax.rem(lax.broadcasted_iota(jnp.int32, vals[0].shape, 0), 8) < 4
    even = [jnp.where(low, p, pltpu.roll(q, 4, 0)) for p, q in (vals[:2], vals[2:])]
    odd = [jnp.where(low, pltpu.roll(p, n - 4, 0), q) for p, q in (vals[:2], vals[2:])]
    for v in range(n // 8):
        at = slice(8 * v, 8 * v + 8)
        for side, both in ((0, even), (1, odd)):
            dst[2 * v + side, pl.ds(slot, 16)] = jnp.concatenate([both[0][at], both[1][at]], axis=0).astype(dst.dtype)


def query_kernel(chips, hid_ref, wq_ref, wr_ref, wk_ref, lat_all, rope_all,
                 wq_buf, wr_buf, wk_buf, wide, acc, lat_own, rope_own, wq_sem, wr_sem, wk_sem, send, recv, local):
    x, c, xr, xl, right, left, partner = place(chips)
    xo = lax.rem(x + 2, chips)
    rows, toks, dim = hid_ref.shape
    pairs, nope = wq_ref.shape[1], wq_ref.shape[3]
    parts = pairs // 2
    depth = dim // CUTS
    f32, bf16 = jnp.float32, jnp.bfloat16

    barrier = pltpu.get_barrier_semaphore()
    for dev in (right, left, partner):
        pl.semaphore_signal(barrier, inc=1, device_id={"seq": dev}, device_id_type=MESH)

    def load(u, k):
        return pltpu.make_async_copy(wq_ref.at[pl.ds(k * depth, depth), u], wq_buf.at[u, pl.ds(k * depth, depth)],
                                     wq_sem.at[u, k])

    def load_rope(half, j):
        return pltpu.make_async_copy(wr_ref.at[half * pairs + j], wr_buf.at[j, half], wr_sem.at[half, j])

    load_up = pltpu.make_async_copy(wk_ref, wk_buf, wk_sem)
    for k in range(CUTS):
        for u in range(2):
            load(u, k).start()
    load_up.start()

    lane = lax.broadcasted_iota(jnp.int32, (128, 512), 1)
    src = lax.broadcasted_iota(jnp.int32, (128, 512), 0)
    spread = jnp.where(lax.rem(lane, 256) == 2 * src + lane // 256, 1.0, 0.0).astype(bf16)
    tiles = depth // 128
    n = rows * toks
    for k in range(CUTS):
        stack = jnp.concatenate([hid_ref[:, :, (k * tiles + t) * 128:(k * tiles + t + 1) * 128].reshape(n, 128)
                                 for t in range(tiles)], axis=0)
        res = jnp.dot(stack, spread, preferred_element_type=f32).astype(bf16)
        for t in range(tiles):
            for side in range(2):
                wide[k, pl.ds(side * n, n), pl.ds(t * 256, 256)] = res[t * n:(t + 1) * n, side * 256:side * 256 + 256]

    where = lambda p: pl.ds((p % parts) * 16, 16)
    own_ref = lambda p: (lat_own if p < parts else rope_own).at[:, where(p)]
    all_ref = lambda p, core, block: (lat_all if p < parts else rope_all).at[:, core, block, where(p)]

    def own(p, kind, dev):
        return remote(own_ref(p), all_ref(p, c, x), send.at[p, kind], recv.at[p, kind], dev)

    def pass_on(p, kind, block, dev):
        return remote(all_ref(p, c, block), all_ref(p, c, block), send.at[p, kind], recv.at[p, kind], dev)

    def landed(p, kind, block, core):
        ref = all_ref(p, core, block)
        return remote(ref, ref, send.at[p, kind], recv.at[p, kind], partner)

    keep = lambda p: pltpu.make_async_copy(own_ref(p), all_ref(p, c, x), local.at[p])

    def send_own(p):
        own(p, 0, right).start()
        own(p, 1, left).start()
        own(p, 2, partner).start()
        keep(p).start()

    def relay(p):
        landed(p, 0, xl, c).wait_recv()
        if p % 2 == 0:
            pass_on(p, 3, xl, right).start()
        pass_on(p, 4, xl, partner).start()
        landed(p, 1, xr, c).wait_recv()
        if p % 2 == 1:
            pass_on(p, 3, xr, left).start()
        pass_on(p, 5, xr, partner).start()

    for q in range(parts):
        acc[...] = jnp.zeros_like(acc)

        @pl.loop(0, CUTS)
        def _(k):
            for u in (2 * q, 2 * q + 1):
                load(u, k).wait()
            if q < parts - 1:
                for u in (2 * q + 2, 2 * q + 3):
                    load(u, k).start()
            if q == parts - 1:
                for half in range(2):
                    load_rope(half, 2 * k).start()
                    load_rope(half, 2 * k + 1).start()
            w = [wq_buf[u, pl.ds(k * depth, depth)].reshape(2 * depth, nope) for u in (2 * q, 2 * q + 1)]
            acc[...] += jnp.dot(wide[k], jnp.concatenate(w, axis=1), preferred_element_type=f32)

        if q == 0:
            load_up.wait()
        q_lat = []
        for h in range(4):
            q_n = acc[pl.ds((h % 2) * n, n), pl.ds((h // 2) * nope, nope)].astype(bf16)
            q_lat.append(jnp.dot(q_n, wk_buf[4 * q + h], preferred_element_type=f32))
        pack(q_lat, lat_own, q * 16)
        if q == 0:
            pl.semaphore_wait(barrier, 3)
        send_own(q)

    tokens = jnp.concatenate([hid_ref[:, :, t * 128:(t + 1) * 128].reshape(n, 128) for t in range(dim // 128)], axis=1)
    for q in range(2):
        q_rope = []
        for m in (2 * q, 2 * q + 1):
            for half in range(2):
                load_rope(half, 2 * m).wait()
                load_rope(half, 2 * m + 1).wait()
            w = wr_buf[pl.ds(2 * m, 2)].reshape(256, dim)
            r = lax.dot_general(tokens, w, (((1,), (1,)), ((), ())), preferred_element_type=f32)
            q_rope += [r[:, 0:128], r[:, 128:256]]
        pack(q_rope, rope_own, 16 * q)
        send_own(parts + q)
    for p in range(parts + 2):
        relay(p)
    for p in range(parts + 2):
        landed(p, 3, xo, c).wait_recv()
        pass_on(p, 6, xo, partner).start()
    for p in range(parts + 2):
        for kind, block in ((2, x), (4, xl), (5, xr), (6, xo)):
            landed(p, kind, block, 1 - c).wait_recv()
        own(p, 0, right).wait_send()
        own(p, 1, left).wait_send()
        own(p, 2, partner).wait_send()
        if p % 2 == 0:
            pass_on(p, 3, xl, right).wait_send()
        else:
            pass_on(p, 3, xr, left).wait_send()
        pass_on(p, 4, xl, partner).wait_send()
        pass_on(p, 5, xr, partner).wait_send()
        pass_on(p, 6, xo, partner).wait_send()
        keep(p).wait()


def queries(chips, hidden, w_uq, w_qr, w_uk):
    rows, toks, dim = hidden.shape
    heads, nope, width = w_uk.shape
    gq = heads * toks
    bf16 = jnp.bfloat16
    wq = w_uq.reshape(dim, heads // 2, 2, nope)
    wr = jnp.transpose(w_qr, (1, 2, 0))
    hbm = pl.BlockSpec(memory_space=pl.ANY)
    dma = pltpu.SemaphoreType.DMA
    return pl.pallas_call(
        functools.partial(query_kernel, chips),
        out_shape=[jax.ShapeDtypeStruct((rows, 2, chips, gq, width), bf16),
                   jax.ShapeDtypeStruct((rows, 2, chips, gq // 2, 128), bf16)],
        in_specs=[pl.BlockSpec(memory_space=pltpu.VMEM), hbm, hbm, hbm],
        out_specs=[hbm] * 2,
        scratch_shapes=[
            pltpu.VMEM((heads // 2, dim, 2, nope), bf16), pltpu.VMEM((heads // 2, 2) + wr.shape[1:], bf16), pltpu.VMEM(w_uk.shape, bf16),
            pltpu.VMEM((CUTS, 2 * rows * toks, 2 * dim // CUTS), bf16),
            pltpu.VMEM((2 * rows * toks, 2 * nope), jnp.float32),
            pltpu.VMEM((rows, gq, width), bf16), pltpu.VMEM((rows, gq // 2, 128), bf16),
            dma((heads // 2, CUTS)), dma((2, heads // 2)), dma(()), dma((heads // 4 + 2, 7)),
            dma((heads // 4 + 2, 7)), dma((heads // 4 + 2,))],
        compiler_params=pltpu.CompilerParams(collective_id=0, has_side_effects=True, vmem_limit_bytes=67_000_000),
        name="make_queries",
    )(hidden, wq, wr, w_uk)


def token(row):
    return lax.rem(row, 4)


def expand(ml):
    col = jnp.transpose(jnp.broadcast_to(ml, (128, 128)))
    return col[0:64, :], col[64:128, :]


def compact(m, l):
    return jnp.transpose(jnp.concatenate([m, l], axis=0))[0:1, :]


def attend_kernel(chips, rows, scale, lens_ref, lat_ref, rope_ref, ckv_ref, kr_ref, out_ref,
                  s_buf, p_buf, away_o, away_ml, home_o, home_ml, d2d_o, d2d_ml, one_o, one_ml, two_o, two_ml,
                  send, recv):
    x, c, xr, xl, right, left, partner = place(chips)
    xo = lax.rem(x + 2, chips)
    i = pl.program_id(0)
    local_len = ckv_ref.shape[1]
    width = ckv_ref.shape[2]
    nq = lat_ref.shape[2]
    gq = nq // chips
    hq = gq // 2
    k2 = scale * LOG2E
    lanes = [pl.ds(j * 128, 128) for j in range(width // 128)]

    def moves(r):
        return (
            (away_o.at[r], d2d_o.at[r], partner),
            (away_ml.at[r], d2d_ml.at[r], partner),
            (home_o.at[r, xo, pl.ds(0, hq)], one_o.at[r, 0], right),
            (home_ml.at[r, xo], one_ml.at[r, 0], right),
            (home_o.at[r, xo, pl.ds(hq, hq)], one_o.at[r, 1], left),
            (home_ml.at[r, xo], one_ml.at[r, 1], left),
            (home_o.at[r, xr], two_o.at[r, 0], right),
            (home_ml.at[r, xr], two_ml.at[r, 0], right),
            (home_o.at[r, xl], two_o.at[r, 1], left),
            (home_ml.at[r, xl], two_ml.at[r, 1], left),
        )

    def copy(r, kind):
        src, dst, dev = moves(r)[kind]
        return remote(src, dst, send.at[r, kind], recv.at[r, kind], dev)

    @pl.when(i == 0)
    def _():
        greet((right, left, partner))

    def late(lag):
        return jnp.where((i >= lag) & (i < rows + lag), i - lag, rows)

    def on_row(lag, act, kinds):
        @pl.when((i >= lag) & (i < rows + lag))
        def _():
            for kind in kinds:
                act(copy(i - lag, kind))

    def merge_pair():
        r = late(LAG_B)
        for g in range(chips):
            ma, la = expand(home_ml[r, g])
            mb, lb = expand(d2d_ml[r, g])
            m = jnp.maximum(ma, mb)
            fa, fb = jnp.exp2((ma - m) * k2), jnp.exp2((mb - m) * k2)
            for at in lanes:
                home_o[r, g, :, at] = home_o[r, g, :, at] * fa + d2d_o[r, g, :, at] * fb
            home_ml[r, g] = compact(m, la * fa + lb * fb)

    def merge_half():
        r = late(LAG_C)
        for side, g in ((0, xr), (1, xl)):
            part = slice(side * hq, (side + 1) * hq)
            ma, la = expand(home_ml[r, g])
            mb, lb = expand(one_ml[r, side])
            m = jnp.maximum(ma, mb)[part]
            fa, fb = jnp.exp2((ma[part] - m) * k2), jnp.exp2((mb[part] - m) * k2)
            for at in lanes:
                home_o[r, g, pl.ds(side * hq, hq), at] = (home_o[r, g, pl.ds(side * hq, hq), at] * fa
                                                          + one_o[r, side, :, at] * fb)
            l = la[part] * fa + lb[part] * fb
            if side == 0:
                m, l = jnp.concatenate([m, ma[hq:]], axis=0), jnp.concatenate([l, la[hq:]], axis=0)
            else:
                m, l = jnp.concatenate([ma[:hq], m], axis=0), jnp.concatenate([la[:hq], l], axis=0)
            home_ml[r, g] = compact(m, l)

    def finish():
        r = late(LAG_D)
        ma, la = expand(home_ml[r, x])
        mb, lb = expand(two_ml[r, 0])
        mc, lc = expand(two_ml[r, 1])
        m = jnp.maximum(ma, jnp.maximum(mb, mc))
        fa, fb, fc = jnp.exp2((ma - m) * k2), jnp.exp2((mb - m) * k2), jnp.exp2((mc - m) * k2)
        l = la * fa + lb * fb + lc * fc
        for at in lanes:
            o = home_o[r, x, :, at] * fa + two_o[r, 0, :, at] * fb + two_o[r, 1, :, at] * fc
            out_ref[0, :, at] = (o / l).astype(out_ref.dtype)

    on_row(LAG_D, lambda cp: cp.wait_recv(), range(6, 10))

    @pl.when(i < rows)
    def _():
        base = (2 * x + c) * local_len
        seen = lens_ref[jnp.minimum(i, rows - 1)] - base
        col = lax.broadcasted_iota(jnp.int32, (nq, local_len), 1)
        tok = token(lax.broadcasted_iota(jnp.int32, (nq, 1), 0))
        visible = col <= seen + tok
        contract = (((1,), (1,)), ((), ()))

        def scores(n, block):
            packed = rope_ref[0, block]
            part = packed.shape[0] // chips
            rope = jnp.concatenate(
                [packed[g * part:(g + 1) * part, h * 64:(h + 1) * 64] for g in range(chips) for h in range(2)], axis=0)
            s = lax.dot_general(lat_ref[0, block], ckv_ref[0], contract, preferred_element_type=jnp.float32)
            s = s + jnp.dot(rope, kr_ref[0], preferred_element_type=jnp.float32)
            s_buf[n] = jnp.where(visible, s, MASK_FILL)

        def weigh(n):
            s = s_buf[n]
            m = jnp.max(s, axis=1, keepdims=True)
            p = jnp.exp2((s - m) * k2)
            l = jnp.sum(p, axis=1, keepdims=True)
            p_buf[n] = p.astype(jnp.bfloat16)
            return m, l

        def mix(n, m, l, o_ref, ml_ref):
            o = jnp.dot(p_buf[n], ckv_ref[0], preferred_element_type=jnp.float32)
            m = jnp.broadcast_to(m, (nq, 128))
            l = jnp.broadcast_to(l, (nq, 128))
            for g in range(chips):
                at = slice(g * gq, (g + 1) * gq)
                o_ref[i, g] = o[at]
                ml_ref[i, g] = compact(m[at], l[at])

        finish()
        scores(0, 1 - c)
        scores(1, c)
        on_row(LAG_B, lambda cp: cp.wait_recv(), range(0, 2))
        on_row(LAG_C, lambda cp: cp.wait_recv(), range(2, 6))
        merge_pair()
        merge_half()
        ml0 = weigh(0)
        mix(0, *ml0, away_o, away_ml)
        ml1 = weigh(1)
        mix(1, *ml1, home_o, home_ml)

    @pl.when(i >= rows)
    def _():
        on_row(LAG_B, lambda cp: cp.wait_recv(), range(0, 2))
        on_row(LAG_C, lambda cp: cp.wait_recv(), range(2, 6))
        merge_pair()
        merge_half()
        finish()

    on_row(0, lambda cp: cp.start(), range(0, 2))
    on_row(LAG_B, lambda cp: cp.start(), range(2, 6))
    on_row(LAG_C, lambda cp: cp.start(), range(6, 10))

    @pl.when(i == rows + LAG_D - 1)
    def _():
        @pl.loop(0, rows)
        def _(r):
            for kind in range(10):
                copy(r, kind).wait_send()


def attend(chips, scale, lens, lat, rope, ckv, kr):
    rows, _, nq, width = lat.shape
    gq = nq // chips
    local_len = ckv.shape[1]
    row = lambda i: jnp.minimum(i, rows - 1)
    f32, bf16 = jnp.float32, jnp.bfloat16
    return pl.pallas_call(
        functools.partial(attend_kernel, chips, rows, scale),
        grid=(rows + LAG_D,),
        out_shape=jax.ShapeDtypeStruct((rows, gq, width), bf16),
        in_specs=[pl.BlockSpec(memory_space=pltpu.SMEM),
                  pl.BlockSpec((1,) + lat.shape[1:], lambda i: (row(i), 0, 0, 0)),
                  pl.BlockSpec((1,) + rope.shape[1:], lambda i: (row(i), 0, 0, 0)),
                  pl.BlockSpec((1,) + ckv.shape[1:], lambda i: (row(i), 0, 0)),
                  pl.BlockSpec((1,) + kr.shape[1:], lambda i: (row(i), 0, 0))],
        out_specs=pl.BlockSpec((1, gq, width), lambda i: (jnp.maximum(i - LAG_D, 0), 0, 0)),
        scratch_shapes=[
            pltpu.VMEM((2, nq, local_len), f32), pltpu.VMEM((2, nq, local_len), bf16),
            pltpu.VMEM((rows + 1, chips, gq, width), f32), pltpu.VMEM((rows + 1, chips, 1, 128), f32),
            pltpu.VMEM((rows + 1, chips, gq, width), f32), pltpu.VMEM((rows + 1, chips, 1, 128), f32),
            pltpu.VMEM((rows + 1, chips, gq, width), f32), pltpu.VMEM((rows + 1, chips, 1, 128), f32),
            pltpu.VMEM((rows + 1, 2, gq // 2, width), f32), pltpu.VMEM((rows + 1, 2, 1, 128), f32),
            pltpu.VMEM((rows + 1, 2, gq, width), f32), pltpu.VMEM((rows + 1, 2, 1, 128), f32),
            pltpu.SemaphoreType.DMA((rows, 10)), pltpu.SemaphoreType.DMA((rows, 10))],
        compiler_params=pltpu.CompilerParams(collective_id=1, has_side_effects=True,
                                             dimension_semantics=("arbitrary",), vmem_limit_bytes=67_000_000),
        name="attend_merge",
    )(lens, lat, rope, ckv, kr)


def unpack(ref, slot):
    rows = ref.shape[0]
    tiles = [ref[b, pl.ds(slot, 16)].astype(jnp.float32) for b in range(rows)]
    vals = []
    for h in range(2):
        even = jnp.concatenate([t[8 * h:8 * h + 8] for t in tiles[0::2]], axis=0)
        odd = jnp.concatenate([t[8 * h:8 * h + 8] for t in tiles[1::2]], axis=0)
        n = even.shape[0]
        low = lax.rem(lax.broadcasted_iota(jnp.int32, even.shape, 0), 8) < 4
        vals += [jnp.where(low, even, pltpu.roll(odd, 4, 0)), jnp.where(low, pltpu.roll(even, n - 4, 0), odd)]
    return [v.astype(ref.dtype) for v in vals]


def output_kernel(chips, o_ref, hid_ref, wv_ref, w_ref, out_ref, o_buf, hid_buf, wv_buf, ov, w_buf,
                  away, near, home, one, two, in_sem, w_sem, send, recv):
    x, c, xr, xl, right, left, partner = place(chips)
    xo = lax.rem(x + 2, chips)
    cols = w_buf.shape[2]
    rows, toks = out_ref.shape[:2]
    span = lambda dev: pl.ds(pl.multiple_of(dev * cols, 128), cols)
    dests = (xo, xr, xl, x)
    order = []
    for k in range(chips):
        order += [2 * dests[k] + 1 - c, 2 * dests[k] + c]

    def load(n):
        return pltpu.make_async_copy(w_ref.at[:, span(order[n])], w_buf.at[n], w_sem.at[n])

    firsts = [pltpu.make_async_copy(o_ref, o_buf, in_sem.at[0]), pltpu.make_async_copy(wv_ref, wv_buf, in_sem.at[1]),
              pltpu.make_async_copy(hid_ref.at[:, :, span(2 * x + c)], hid_buf, in_sem.at[2])]
    for cp in firsts:
        cp.start()
    for n in range(AHEAD):
        load(n).start()
    greet((right, left, partner))

    firsts[0].wait()
    firsts[1].wait()
    value = wv_buf.shape[2]
    for q in range(wv_buf.shape[0] // 4):
        for h, o_lat in enumerate(unpack(o_buf, 16 * q)):
            ov[:, pl.ds((4 * q + h) * value, value)] = jnp.dot(
                o_lat, wv_buf[4 * q + h], preferred_element_type=jnp.float32).astype(ov.dtype)

    tokens = ov.shape[0]
    first, second = pl.ds(0, tokens // 2), pl.ds(tokens // 2, tokens // 2)

    def project(n):
        load(n).wait()
        if n + AHEAD < 2 * chips:
            load(n + AHEAD).start()
        return jnp.dot(ov[...], w_buf[n], preferred_element_type=jnp.float32)

    def swap(k):
        return remote(away.at[k], near.at[k], send.at[0, k], recv.at[0, k], partner)

    def hop(kind):
        src, dst, dev = ((home.at[0, first], one.at[0], right), (home.at[0, second], one.at[1], left),
                         (home.at[1], two.at[0], right), (home.at[2], two.at[1], left))[kind]
        return remote(src, dst, send.at[1, kind], recv.at[1, kind], dev)

    away[0] = project(0)
    swap(0).start()
    for k in range(chips):
        home[k] = project(2 * k + 1)
        if k + 1 < chips:
            away[k + 1] = project(2 * k + 2)
            swap(k + 1).start()
        swap(k).wait_recv()
        home[k] = home[k] + near[k]
        if k == 0:
            hop(0).start()
            hop(1).start()
        if k == 1:
            hop(0).wait_recv()
            home[1, first] = home[1, first] + one[0]
            hop(2).start()
        if k == 2:
            hop(1).wait_recv()
            home[2, second] = home[2, second] + one[1]
            hop(3).start()
    firsts[2].wait()
    hop(2).wait_recv()
    hop(3).wait_recv()
    y = home[chips - 1] + two[0] + two[1]
    out_ref[:, :, span(2 * x + c)] = (hid_buf[...].astype(jnp.float32) + y.reshape(rows, toks, cols)).astype(out_ref.dtype)

    whole, top, low = pl.ds(0, rows), pl.ds(0, rows // 2), pl.ds(rows // 2, rows // 2)

    def give(kind, part, block, core, dev):
        ref = out_ref.at[part, :, span(2 * block + core)]
        return remote(ref, ref, send.at[2, kind], recv.at[2, kind], dev)

    sends = [give(0, whole, x, c, right), give(1, whole, x, c, left), give(2, whole, x, c, partner),
             give(3, top, xl, c, right), give(4, low, xr, c, left),
             give(5, whole, xl, c, partner), give(6, whole, xr, c, partner),
             give(7, top, xo, c, partner), give(8, low, xo, c, partner)]
    for n in (0, 1, 2):
        sends[n].start()
    give(0, whole, xl, c, partner).wait_recv()
    sends[3].start()
    sends[5].start()
    give(1, whole, xr, c, partner).wait_recv()
    sends[4].start()
    sends[6].start()
    give(3, top, xo, c, partner).wait_recv()
    sends[7].start()
    give(4, low, xo, c, partner).wait_recv()
    sends[8].start()
    for kind, part, block in ((2, whole, x), (5, whole, xl), (6, whole, xr), (7, top, xo), (8, low, xo)):
        give(kind, part, block, 1 - c, partner).wait_recv()
    for k in range(chips):
        swap(k).wait_send()
        hop(k).wait_send()
    for cp in sends:
        cp.wait_send()


def output(chips, o_lat, hidden, w_uv, w_o):
    rows, toks, dim = hidden.shape
    tokens = rows * toks
    depth = w_o.shape[0]
    cols = dim // (2 * chips)
    f32 = jnp.float32
    vmem, hbm = pl.BlockSpec(memory_space=pltpu.VMEM), pl.BlockSpec(memory_space=pl.ANY)
    dma = pltpu.SemaphoreType.DMA
    return pl.pallas_call(
        functools.partial(output_kernel, chips),
        out_shape=jax.ShapeDtypeStruct(hidden.shape, hidden.dtype),
        in_specs=[hbm] * 4,
        out_specs=vmem,
        scratch_shapes=[
            pltpu.VMEM(o_lat.shape, o_lat.dtype), pltpu.VMEM((rows, toks, cols), hidden.dtype),
            pltpu.VMEM(w_uv.shape, w_uv.dtype), pltpu.VMEM((tokens, depth), o_lat.dtype),
            pltpu.VMEM((2 * chips, depth, cols), w_o.dtype),
            pltpu.VMEM((chips, tokens, cols), f32), pltpu.VMEM((chips, tokens, cols), f32),
            pltpu.VMEM((chips, tokens, cols), f32), pltpu.VMEM((2, tokens // 2, cols), f32),
            pltpu.VMEM((2, tokens, cols), f32),
            dma((3,)), dma((2 * chips,)), dma((3, 9)), dma((3, 9))],
        compiler_params=pltpu.CompilerParams(collective_id=2, has_side_effects=True, vmem_limit_bytes=60_000_000),
        name="project_output",
    )(o_lat, hidden, w_uv, w_o)


def solution(mesh):
    chips = mesh.shape["seq"] // 2

    def local_step(hidden, cache_lens, c_kv, k_r, w_uq, w_qr, w_uk, w_uv, w_o):
        rows, toks, dim = hidden.shape
        heads, nope, width = w_uk.shape
        rope_dim = w_qr.shape[2]
        value = w_uv.shape[2]
        score_scale = (nope + rope_dim) ** -0.5
        gq = toks * heads
        lat_all, rope_all = queries(chips, hidden, w_uq, w_qr, w_uk)
        o_lat = attend(chips, score_scale, cache_lens,
                       lat_all.reshape(rows, 2, chips * gq, width),
                       rope_all.reshape(rows, 2, chips * gq // 2, 2 * rope_dim), c_kv, jnp.swapaxes(k_r, 1, 2))
        return output(chips, o_lat, hidden, w_uv, w_o.reshape(heads * value, dim))

    specs_in = (P("batch", None, None), P("batch"), P("batch", "seq", None), P("batch", "seq", None),
                P(None, "seq", None), P(None, "seq", None), P("seq", None, None), P("seq", None, None),
                P("seq", None, None))
    return jax.shard_map(local_step, mesh=mesh, in_specs=specs_in, out_specs=P("batch", None, None), check_vma=False)
```

```python
import functools

import jax
import jax.numpy as jnp
from jax import lax
from jax.experimental import pallas as pl
from jax.experimental.pallas import tpu as pltpu
from jax.sharding import PartitionSpec as P

MASK_FILL = -1e30
LOG2E = 1.4426950408889634
MESH = pl.DeviceIdType.MESH
LAG_B, LAG_C, LAG_D = 1, 3, 6
CUTS = 4
AHEAD = 3
AWAY, HOME, PAIR, ONE, TWO = 4, 10, 4, 6, 8


def remote(src, dst, send_sem, recv_sem, dev):
    return pltpu.make_async_remote_copy(src_ref=src, dst_ref=dst, send_sem=send_sem, recv_sem=recv_sem,
                                        device_id={"seq": dev}, device_id_type=MESH)


def place(chips):
    me = lax.axis_index("seq")
    x, c = me // 2, lax.rem(me, 2)
    xr, xl = lax.rem(x + 1, chips), lax.rem(x + chips - 1, chips)
    return x, c, xr, xl, 2 * xr + c, 2 * xl + c, 2 * x + 1 - c


def greet(devs):
    barrier = pltpu.get_barrier_semaphore()
    for dev in devs:
        pl.semaphore_signal(barrier, inc=1, device_id={"seq": dev}, device_id_type=MESH)
    pl.semaphore_wait(barrier, len(devs))


def pack(vals, dst, slot):
    n = vals[0].shape[0]
    low = lax.rem(lax.broadcasted_iota(jnp.int32, vals[0].shape, 0), 8) < 4
    even = [jnp.where(low, p, pltpu.roll(q, 4, 0)) for p, q in (vals[:2], vals[2:])]
    odd = [jnp.where(low, pltpu.roll(p, n - 4, 0), q) for p, q in (vals[:2], vals[2:])]
    for v in range(n // 8):
        at = slice(8 * v, 8 * v + 8)
        for side, both in ((0, even), (1, odd)):
            dst[2 * v + side, pl.ds(slot, 16)] = jnp.concatenate([both[0][at], both[1][at]], axis=0).astype(dst.dtype)


def token(row):
    return lax.rem(row, 4)


def expand(ml):
    col = jnp.transpose(jnp.broadcast_to(ml, (128, 128)))
    return col[0:64, :], col[64:128, :]


def compact(m, l):
    return jnp.transpose(jnp.concatenate([m, l], axis=0))[0:1, :]


def attend_kernel(chips, rows, scale, lens_ref, hid_ref, wq_ref, wr_ref, wk_ref, ckv_ref, kr_ref, out_ref,
                  wq_buf, wr_buf, wk_buf, wide, acc, lat_all, rope_all, s_buf, p_buf,
                  away_o, away_ml, home_o, home_ml, d2d_o, d2d_ml, one_o, one_ml, two_o, two_ml,
                  wq_sem, wr_sem, wk_sem, q_send, q_recv, send, recv):
    x, c, xr, xl, right, left, partner = place(chips)
    xo = lax.rem(x + 2, chips)
    i = pl.program_id(0)
    f32, bf16 = jnp.float32, jnp.bfloat16
    toks, dim = hid_ref.shape[1:]
    n = rows * toks
    pairs, nope = wq_ref.shape[1], wq_ref.shape[3]
    quarters = pairs // 2
    depth = dim // CUTS
    local_len, width = ckv_ref.shape[1:]
    gq = lat_all.shape[3]
    nq = chips * gq
    hq = gq // 2
    k2 = scale * LOG2E
    lanes = [pl.ds(j * 128, 128) for j in range(width // 128)]

    top, low, every = pl.ds(0, rows // 2), pl.ds(rows // 2, rows // 2), pl.ds(0, rows)
    pieces = [(lat_all, every, pl.ds(0, 16), 0), (lat_all, every, pl.ds(16, 16), 1)]
    for part, turn in ((top, 0), (low, 1)):
        pieces += [(lat_all, part, pl.ds(32, 16), 0), (lat_all, part, pl.ds(48, 16), 1),
                   (rope_all, part, pl.ds(0, hq), turn)]

    def give(p, kind, block, core, dev):
        array, part, queries, _ = pieces[p]
        ref = array.at[part, core, block, queries]
        return remote(ref, ref, q_send.at[p, kind], q_recv.at[p, kind], dev)

    def send_own(p):
        give(p, 0, x, c, right).start()
        give(p, 1, x, c, left).start()
        give(p, 2, x, c, partner).start()

    def second_hop(p):
        return give(p, 3, xr, c, left) if pieces[p][3] else give(p, 3, xl, c, right)

    def relay(p):
        give(p, 0, xl, c, partner).wait_recv()
        if pieces[p][3] == 0:
            second_hop(p).start()
        give(p, 4, xl, c, partner).start()
        give(p, 1, xr, c, partner).wait_recv()
        if pieces[p][3] == 1:
            second_hop(p).start()
        give(p, 5, xr, c, partner).start()

    def relay_far(p):
        give(p, 3, xo, c, partner).wait_recv()
        give(p, 6, xo, c, partner).start()

    def complete(p):
        for kind, block in ((2, x), (4, xl), (5, xr), (6, xo)):
            give(p, kind, block, 1 - c, partner).wait_recv()

    def sent(p):
        give(p, 0, x, c, right).wait_send()
        give(p, 1, x, c, left).wait_send()
        give(p, 2, x, c, partner).wait_send()
        second_hop(p).wait_send()
        give(p, 4, xl, c, partner).wait_send()
        give(p, 5, xr, c, partner).wait_send()
        give(p, 6, xo, c, partner).wait_send()

    def make_queries():
        barrier = pltpu.get_barrier_semaphore()
        for dev in (right, left, partner):
            pl.semaphore_signal(barrier, inc=1, device_id={"seq": dev}, device_id_type=MESH)

        def load(q, h, k):
            at = pl.ds(k * depth, depth)
            return pltpu.make_async_copy(wq_ref.at[at, 2 * q + h], wq_buf.at[h, at], wq_sem.at[q, h, k])

        def load_rope(half, j):
            return pltpu.make_async_copy(wr_ref.at[half * pairs + j], wr_buf.at[j % 4, half], wr_sem.at[half, j])

        load_up = pltpu.make_async_copy(wk_ref, wk_buf, wk_sem)
        for k in range(CUTS):
            for h in range(2):
                load(0, h, k).start()
        load_up.start()
        for j in range(4):
            for half in range(2):
                load_rope(half, j).start()

        lane = lax.broadcasted_iota(jnp.int32, (128, 512), 1)
        src = lax.broadcasted_iota(jnp.int32, (128, 512), 0)
        spread = jnp.where(lax.rem(lane, 256) == 2 * src + lane // 256, 1.0, 0.0).astype(bf16)
        tiles = depth // 128
        for k in range(CUTS):
            stack = jnp.concatenate([hid_ref[:, :, (k * tiles + t) * 128:(k * tiles + t + 1) * 128].reshape(n, 128)
                                     for t in range(tiles)], axis=0)
            res = jnp.dot(stack, spread, preferred_element_type=f32).astype(bf16)
            for t in range(tiles):
                for side in range(2):
                    wide[k, pl.ds(side * n, n), pl.ds(t * 256, 256)] = res[t * n:(t + 1) * n,
                                                                           side * 256:side * 256 + 256]

        for q in range(quarters):
            acc[...] = jnp.zeros_like(acc)

            @pl.loop(0, CUTS)
            def _(k):
                for h in range(2):
                    load(q, h, k).wait()
                w = [wq_buf[h, pl.ds(k * depth, depth)].reshape(2 * depth, nope) for h in range(2)]
                acc[...] += jnp.dot(wide[k], jnp.concatenate(w, axis=1), preferred_element_type=f32)
                if q < quarters - 1:
                    for h in range(2):
                        load(q + 1, h, k).start()

            if q == 0:
                load_up.wait()
            q_lat = []
            for h in range(4):
                q_n = acc[pl.ds((h % 2) * n, n), pl.ds((h // 2) * nope, nope)].astype(bf16)
                q_lat.append(jnp.dot(q_n, wk_buf[4 * q + h], preferred_element_type=f32))
            pack(q_lat, lat_all.at[:, c, x], q * 16)
            if q == 0:
                pl.semaphore_wait(barrier, 3)
            send_own(q)

        tokens = jnp.concatenate([hid_ref[:, :, t * 128:(t + 1) * 128].reshape(n, 128) for t in range(dim // 128)],
                                 axis=1)
        for q in range(2):
            q_rope = []
            for m in (2 * q, 2 * q + 1):
                for half in range(2):
                    load_rope(half, 2 * m).wait()
                    load_rope(half, 2 * m + 1).wait()
                w = wr_buf[pl.ds(2 * m % 4, 2)].reshape(256, dim)
                r = lax.dot_general(tokens, w, (((1,), (1,)), ((), ())), preferred_element_type=f32)
                if q == 0:
                    for half in range(2):
                        load_rope(half, 2 * m + 4).start()
                        load_rope(half, 2 * m + 5).start()
                q_rope += [r[:, 0:128], r[:, 128:256]]
            pack(q_rope, rope_all.at[:, c, x], 16 * q)
        send_own(4)
        for p in range(5):
            relay(p)
        for p in range(5, 8):
            send_own(p)
        for p in range(5):
            relay_far(p)
        for p in range(5):
            complete(p)

    def moves(r):
        a, h, d, e, t = (lax.rem(r, count) for count in (AWAY, HOME, PAIR, ONE, TWO))
        return (
            (away_o.at[a], d2d_o.at[d], partner),
            (away_ml.at[r], d2d_ml.at[r], partner),
            (home_o.at[h, xo, pl.ds(0, hq)], one_o.at[e, 0], right),
            (home_ml.at[r, xo], one_ml.at[r, 0], right),
            (home_o.at[h, xo, pl.ds(hq, hq)], one_o.at[e, 1], left),
            (home_ml.at[r, xo], one_ml.at[r, 1], left),
            (home_o.at[h, xr], two_o.at[t, 0], right),
            (home_ml.at[r, xr], two_ml.at[r, 0], right),
            (home_o.at[h, xl], two_o.at[t, 1], left),
            (home_ml.at[r, xl], two_ml.at[r, 1], left),
        )

    def copy(r, kind):
        src, dst, dev = moves(r)[kind]
        return remote(src, dst, send.at[r, kind], recv.at[r, kind], dev)

    def late(lag):
        return jnp.where((i >= lag) & (i < rows + lag), i - lag, rows)

    def slot(r, count):
        return jnp.where(r < rows, lax.rem(r, count), count)

    def on_row(lag, act, kinds):
        @pl.when((i >= lag) & (i < rows + lag))
        def _():
            for kind in kinds:
                act(copy(i - lag, kind))

    def merge_pair():
        r = late(LAG_B)
        h, d = slot(r, HOME), slot(r, PAIR)
        for g in range(chips):
            ma, la = expand(home_ml[r, g])
            mb, lb = expand(d2d_ml[r, g])
            m = jnp.maximum(ma, mb)
            fa, fb = jnp.exp2((ma - m) * k2), jnp.exp2((mb - m) * k2)
            for at in lanes:
                home_o[h, g, :, at] = home_o[h, g, :, at] * fa + d2d_o[d, g, :, at] * fb
            home_ml[r, g] = compact(m, la * fa + lb * fb)

    def merge_half():
        r = late(LAG_C)
        h, e = slot(r, HOME), slot(r, ONE)
        for side, g in ((0, xr), (1, xl)):
            part = slice(side * hq, (side + 1) * hq)
            ma, la = expand(home_ml[r, g])
            mb, lb = expand(one_ml[r, side])
            m = jnp.maximum(ma, mb)[part]
            fa, fb = jnp.exp2((ma[part] - m) * k2), jnp.exp2((mb[part] - m) * k2)
            for at in lanes:
                home_o[h, g, pl.ds(side * hq, hq), at] = (home_o[h, g, pl.ds(side * hq, hq), at] * fa
                                                          + one_o[e, side, :, at] * fb)
            l = la[part] * fa + lb[part] * fb
            if side == 0:
                m, l = jnp.concatenate([m, ma[hq:]], axis=0), jnp.concatenate([l, la[hq:]], axis=0)
            else:
                m, l = jnp.concatenate([ma[:hq], m], axis=0), jnp.concatenate([la[:hq], l], axis=0)
            home_ml[r, g] = compact(m, l)

    def finish():
        r = late(LAG_D)
        h, e = slot(r, HOME), slot(r, TWO)
        ma, la = expand(home_ml[r, x])
        mb, lb = expand(two_ml[r, 0])
        mc, lc = expand(two_ml[r, 1])
        m = jnp.maximum(ma, jnp.maximum(mb, mc))
        fa, fb, fc = jnp.exp2((ma - m) * k2), jnp.exp2((mb - m) * k2), jnp.exp2((mc - m) * k2)
        l = la * fa + lb * fb + lc * fc
        for at in lanes:
            o = home_o[h, x, :, at] * fa + two_o[e, 0, :, at] * fb + two_o[e, 1, :, at] * fc
            out_ref[0, :, at] = (o / l).astype(out_ref.dtype)

    @pl.when(i == 0)
    def _():
        make_queries()

    @pl.when(i == rows // 2)
    def _():
        for p in range(5, 8):
            complete(p)

    @pl.when((i >= AWAY) & (i < rows + AWAY))
    def _():
        for kind in range(0, 2):
            copy(i - AWAY, kind).wait_send()

    @pl.when(i >= HOME)
    def _():
        for kind in range(2, 10):
            copy(i - HOME, kind).wait_send()

    on_row(LAG_D, lambda cp: cp.wait_recv(), range(6, 10))

    @pl.when(i < rows)
    def _():
        base = (2 * x + c) * local_len
        row = jnp.minimum(i, rows - 1)
        seen = lens_ref[row] - base
        a, h = lax.rem(row, AWAY), lax.rem(row, HOME)
        col = lax.broadcasted_iota(jnp.int32, (nq, local_len), 1)
        tok = token(lax.broadcasted_iota(jnp.int32, (nq, 1), 0))
        visible = col <= seen + tok
        contract = (((1,), (1,)), ((), ()))

        def scores(k, block):
            lat = lat_all[row, block].reshape(nq, width)
            rope = jnp.concatenate([rope_all[row, block, g][:, e * 64:(e + 1) * 64] for g in range(chips) for e in range(2)],
                                   axis=0)
            s = lax.dot_general(lat, ckv_ref[0], contract, preferred_element_type=f32)
            s = s + jnp.dot(rope, kr_ref[0], preferred_element_type=f32)
            s_buf[k] = jnp.where(visible, s, MASK_FILL)

        def weigh(k):
            s = s_buf[k]
            m = jnp.max(s, axis=1, keepdims=True)
            p = jnp.exp2((s - m) * k2)
            l = jnp.sum(p, axis=1, keepdims=True)
            p_buf[k] = p.astype(bf16)
            return m, l

        def mix(k, m, l, o_ref, to, ml_ref):
            o = jnp.dot(p_buf[k], ckv_ref[0], preferred_element_type=f32)
            m = jnp.broadcast_to(m, (nq, 128))
            l = jnp.broadcast_to(l, (nq, 128))
            for g in range(chips):
                at = slice(g * gq, (g + 1) * gq)
                o_ref[to, g] = o[at]
                ml_ref[row, g] = compact(m[at], l[at])

        finish()
        scores(0, 1 - c)
        scores(1, c)
        on_row(LAG_B, lambda cp: cp.wait_recv(), range(0, 2))
        on_row(LAG_C, lambda cp: cp.wait_recv(), range(2, 6))
        merge_pair()
        merge_half()
        ml0 = weigh(0)
        mix(0, *ml0, away_o, a, away_ml)
        ml1 = weigh(1)
        mix(1, *ml1, home_o, h, home_ml)

    @pl.when(i >= rows)
    def _():
        on_row(LAG_B, lambda cp: cp.wait_recv(), range(0, 2))
        on_row(LAG_C, lambda cp: cp.wait_recv(), range(2, 6))
        merge_pair()
        merge_half()
        finish()

    on_row(0, lambda cp: cp.start(), range(0, 2))
    on_row(LAG_B, lambda cp: cp.start(), range(2, 6))
    on_row(LAG_C, lambda cp: cp.start(), range(6, 10))

    @pl.when(i == 0)
    def _():
        relay(5)

    @pl.when(i == 1)
    def _():
        relay(6)
        relay(7)

    @pl.when(i == 3)
    def _():
        for p in range(5, 8):
            relay_far(p)

    @pl.when(i == rows + LAG_D - 1)
    def _():
        for p in range(8):
            sent(p)

        @pl.loop(rows + LAG_D - HOME, rows)
        def _(r):
            for kind in range(2, 10):
                copy(r, kind).wait_send()


def attend(chips, scale, lens, hidden, w_uq, w_qr, w_uk, ckv, kr):
    rows, toks, dim = hidden.shape
    heads, nope, width = w_uk.shape
    gq = heads * toks
    nq = chips * gq
    local_len = ckv.shape[1]
    wq = w_uq.reshape(dim, heads // 2, 2, nope)
    wr = jnp.transpose(w_qr, (1, 2, 0))
    row = lambda i: jnp.minimum(i, rows - 1)
    f32, bf16 = jnp.float32, jnp.bfloat16
    hbm = pl.BlockSpec(memory_space=pl.ANY)
    dma = pltpu.SemaphoreType.DMA
    return pl.pallas_call(
        functools.partial(attend_kernel, chips, rows, scale),
        grid=(rows + LAG_D,),
        out_shape=jax.ShapeDtypeStruct((rows, gq, width), bf16),
        in_specs=[pl.BlockSpec(memory_space=pltpu.SMEM), pl.BlockSpec(memory_space=pltpu.VMEM), hbm, hbm, hbm,
                  pl.BlockSpec((1,) + ckv.shape[1:], lambda i: (row(i), 0, 0)),
                  pl.BlockSpec((1,) + kr.shape[1:], lambda i: (row(i), 0, 0))],
        out_specs=pl.BlockSpec((1, gq, width), lambda i: (jnp.maximum(i - LAG_D, 0), 0, 0)),
        scratch_shapes=[
            pltpu.VMEM((2, dim, 2, nope), bf16), pltpu.VMEM((4, 2) + wr.shape[1:], bf16), pltpu.VMEM(w_uk.shape, bf16),
            pltpu.VMEM((CUTS, 2 * rows * toks, 2 * dim // CUTS), bf16), pltpu.VMEM((2 * rows * toks, 2 * nope), f32),
            pltpu.VMEM((rows, 2, chips, gq, width), bf16), pltpu.VMEM((rows, 2, chips, gq // 2, 128), bf16),
            pltpu.VMEM((2, nq, local_len), f32), pltpu.VMEM((2, nq, local_len), bf16),
            pltpu.VMEM((AWAY, chips, gq, width), f32), pltpu.VMEM((rows + 1, chips, 1, 128), f32),
            pltpu.VMEM((HOME + 1, chips, gq, width), f32), pltpu.VMEM((rows + 1, chips, 1, 128), f32),
            pltpu.VMEM((PAIR + 1, chips, gq, width), f32), pltpu.VMEM((rows + 1, chips, 1, 128), f32),
            pltpu.VMEM((ONE + 1, 2, gq // 2, width), f32), pltpu.VMEM((rows + 1, 2, 1, 128), f32),
            pltpu.VMEM((TWO + 1, 2, gq, width), f32), pltpu.VMEM((rows + 1, 2, 1, 128), f32),
            dma((heads // 4, 2, CUTS)), dma((2, heads // 2)), dma(()), dma((8, 7)), dma((8, 7)),
            dma((rows, 10)), dma((rows, 10))],
        compiler_params=pltpu.CompilerParams(collective_id=1, has_side_effects=True,
                                             dimension_semantics=("arbitrary",), vmem_limit_bytes=67_000_000),
        name="attend_merge",
    )(lens, hidden, wq, wr, w_uk, ckv, kr)


def unpack(ref, slot):
    rows = ref.shape[0]
    tiles = [ref[b, pl.ds(slot, 16)].astype(jnp.float32) for b in range(rows)]
    vals = []
    for h in range(2):
        even = jnp.concatenate([t[8 * h:8 * h + 8] for t in tiles[0::2]], axis=0)
        odd = jnp.concatenate([t[8 * h:8 * h + 8] for t in tiles[1::2]], axis=0)
        n = even.shape[0]
        low = lax.rem(lax.broadcasted_iota(jnp.int32, even.shape, 0), 8) < 4
        vals += [jnp.where(low, even, pltpu.roll(odd, 4, 0)), jnp.where(low, pltpu.roll(even, n - 4, 0), odd)]
    return [v.astype(ref.dtype) for v in vals]


def output_kernel(chips, o_ref, hid_ref, wv_ref, w_ref, out_ref, o_buf, hid_buf, wv_buf, ov, w_buf,
                  away, near, home, one, two, in_sem, w_sem, send, recv):
    x, c, xr, xl, right, left, partner = place(chips)
    xo = lax.rem(x + 2, chips)
    cols = w_buf.shape[2]
    rows, toks = out_ref.shape[:2]
    span = lambda dev: pl.ds(pl.multiple_of(dev * cols, 128), cols)
    dests = (xo, xr, xl, x)
    order = []
    for k in range(chips):
        order += [2 * dests[k] + 1 - c, 2 * dests[k] + c]

    def load(n):
        return pltpu.make_async_copy(w_ref.at[:, span(order[n])], w_buf.at[n], w_sem.at[n])

    firsts = [pltpu.make_async_copy(o_ref, o_buf, in_sem.at[0]), pltpu.make_async_copy(wv_ref, wv_buf, in_sem.at[1]),
              pltpu.make_async_copy(hid_ref.at[:, :, span(2 * x + c)], hid_buf, in_sem.at[2])]
    for cp in firsts:
        cp.start()
    for n in range(AHEAD):
        load(n).start()
    greet((right, left, partner))

    firsts[0].wait()
    firsts[1].wait()
    value = wv_buf.shape[2]
    for q in range(wv_buf.shape[0] // 4):
        for h, o_lat in enumerate(unpack(o_buf, 16 * q)):
            ov[:, pl.ds((4 * q + h) * value, value)] = jnp.dot(
                o_lat, wv_buf[4 * q + h], preferred_element_type=jnp.float32).astype(ov.dtype)

    tokens = ov.shape[0]
    first, second = pl.ds(0, tokens // 2), pl.ds(tokens // 2, tokens // 2)

    def project(n):
        load(n).wait()
        if n + AHEAD < 2 * chips:
            load(n + AHEAD).start()
        return jnp.dot(ov[...], w_buf[n], preferred_element_type=jnp.float32)

    def swap(k):
        return remote(away.at[k], near.at[k], send.at[0, k], recv.at[0, k], partner)

    def hop(kind):
        src, dst, dev = ((home.at[0, first], one.at[0], right), (home.at[0, second], one.at[1], left),
                         (home.at[1], two.at[0], right), (home.at[2], two.at[1], left))[kind]
        return remote(src, dst, send.at[1, kind], recv.at[1, kind], dev)

    away[0] = project(0)
    swap(0).start()
    for k in range(chips):
        home[k] = project(2 * k + 1)
        if k + 1 < chips:
            away[k + 1] = project(2 * k + 2)
            swap(k + 1).start()
        swap(k).wait_recv()
        home[k] = home[k] + near[k]
        if k == 0:
            hop(0).start()
            hop(1).start()
        if k == 1:
            hop(0).wait_recv()
            home[1, first] = home[1, first] + one[0]
            hop(2).start()
        if k == 2:
            hop(1).wait_recv()
            home[2, second] = home[2, second] + one[1]
            hop(3).start()
    firsts[2].wait()
    hop(2).wait_recv()
    hop(3).wait_recv()
    y = home[chips - 1] + two[0] + two[1]
    out_ref[:, :, span(2 * x + c)] = (hid_buf[...].astype(jnp.float32) + y.reshape(rows, toks, cols)).astype(out_ref.dtype)

    whole, top, low = pl.ds(0, rows), pl.ds(0, rows // 2), pl.ds(rows // 2, rows // 2)

    def give(kind, part, block, core, dev):
        ref = out_ref.at[part, :, span(2 * block + core)]
        return remote(ref, ref, send.at[2, kind], recv.at[2, kind], dev)

    sends = [give(0, whole, x, c, right), give(1, whole, x, c, left), give(2, whole, x, c, partner),
             give(3, top, xl, c, right), give(4, low, xr, c, left),
             give(5, whole, xl, c, partner), give(6, whole, xr, c, partner),
             give(7, top, xo, c, partner), give(8, low, xo, c, partner)]
    for n in (0, 1, 2):
        sends[n].start()
    give(0, whole, xl, c, partner).wait_recv()
    sends[3].start()
    sends[5].start()
    give(1, whole, xr, c, partner).wait_recv()
    sends[4].start()
    sends[6].start()
    give(3, top, xo, c, partner).wait_recv()
    sends[7].start()
    give(4, low, xo, c, partner).wait_recv()
    sends[8].start()
    for kind, part, block in ((2, whole, x), (5, whole, xl), (6, whole, xr), (7, top, xo), (8, low, xo)):
        give(kind, part, block, 1 - c, partner).wait_recv()
    for k in range(chips):
        swap(k).wait_send()
        hop(k).wait_send()
    for cp in sends:
        cp.wait_send()


def output(chips, o_lat, hidden, w_uv, w_o):
    rows, toks, dim = hidden.shape
    tokens = rows * toks
    depth = w_o.shape[0]
    cols = dim // (2 * chips)
    f32 = jnp.float32
    vmem, hbm = pl.BlockSpec(memory_space=pltpu.VMEM), pl.BlockSpec(memory_space=pl.ANY)
    dma = pltpu.SemaphoreType.DMA
    return pl.pallas_call(
        functools.partial(output_kernel, chips),
        out_shape=jax.ShapeDtypeStruct(hidden.shape, hidden.dtype),
        in_specs=[hbm] * 4,
        out_specs=vmem,
        scratch_shapes=[
            pltpu.VMEM(o_lat.shape, o_lat.dtype), pltpu.VMEM((rows, toks, cols), hidden.dtype),
            pltpu.VMEM(w_uv.shape, w_uv.dtype), pltpu.VMEM((tokens, depth), o_lat.dtype),
            pltpu.VMEM((2 * chips, depth, cols), w_o.dtype),
            pltpu.VMEM((chips, tokens, cols), f32), pltpu.VMEM((chips, tokens, cols), f32),
            pltpu.VMEM((chips, tokens, cols), f32), pltpu.VMEM((2, tokens // 2, cols), f32),
            pltpu.VMEM((2, tokens, cols), f32),
            dma((3,)), dma((2 * chips,)), dma((3, 9)), dma((3, 9))],
        compiler_params=pltpu.CompilerParams(collective_id=2, has_side_effects=True, vmem_limit_bytes=60_000_000),
        name="project_output",
    )(o_lat, hidden, w_uv, w_o)


def solution(mesh):
    chips = mesh.shape["seq"] // 2

    def local_step(hidden, cache_lens, c_kv, k_r, w_uq, w_qr, w_uk, w_uv, w_o):
        rows, toks, dim = hidden.shape
        heads, nope, width = w_uk.shape
        rope_dim = w_qr.shape[2]
        value = w_uv.shape[2]
        score_scale = (nope + rope_dim) ** -0.5
        o_lat = attend(chips, score_scale, cache_lens, hidden, w_uq, w_qr, w_uk, c_kv, jnp.swapaxes(k_r, 1, 2))
        return output(chips, o_lat, hidden, w_uv, w_o.reshape(heads * value, dim))

    specs_in = (P("batch", None, None), P("batch"), P("batch", "seq", None), P("batch", "seq", None),
                P(None, "seq", None), P(None, "seq", None), P("seq", None, None), P("seq", None, None),
                P("seq", None, None))
    return jax.shard_map(local_step, mesh=mesh, in_specs=specs_in, out_specs=P("batch", None, None), check_vma=False)
```

```python
import functools

import jax
import jax.numpy as jnp
from jax import lax
from jax.experimental import pallas as pl
from jax.experimental.pallas import tpu as pltpu
from jax.sharding import PartitionSpec as P

MASK_FILL = -1e30
LOG2E = 1.4426950408889634
MESH = pl.DeviceIdType.MESH
LAG_B, LAG_C, LAG_D = 1, 3, 6
CUTS = 4
AHEAD = 3
AWAY, HOME, PAIR, ONE, TWO = 4, 10, 4, 4, 6


def remote(src, dst, send_sem, recv_sem, dev):
    return pltpu.make_async_remote_copy(src_ref=src, dst_ref=dst, send_sem=send_sem, recv_sem=recv_sem,
                                        device_id={"seq": dev}, device_id_type=MESH)


def place(chips):
    me = lax.axis_index("seq")
    x, c = me // 2, lax.rem(me, 2)
    xr, xl = lax.rem(x + 1, chips), lax.rem(x + chips - 1, chips)
    return x, c, xr, xl, 2 * xr + c, 2 * xl + c, 2 * x + 1 - c


def greet(devs):
    barrier = pltpu.get_barrier_semaphore()
    for dev in devs:
        pl.semaphore_signal(barrier, inc=1, device_id={"seq": dev}, device_id_type=MESH)
    pl.semaphore_wait(barrier, len(devs))


def pack(vals, dst, slot):
    n = vals[0].shape[0]
    low = lax.rem(lax.broadcasted_iota(jnp.int32, vals[0].shape, 0), 8) < 4
    even = [jnp.where(low, p, pltpu.roll(q, 4, 0)) for p, q in (vals[:2], vals[2:])]
    odd = [jnp.where(low, pltpu.roll(p, n - 4, 0), q) for p, q in (vals[:2], vals[2:])]
    for v in range(n // 8):
        at = slice(8 * v, 8 * v + 8)
        for side, both in ((0, even), (1, odd)):
            dst[2 * v + side, pl.ds(slot, 16)] = jnp.concatenate([both[0][at], both[1][at]], axis=0).astype(dst.dtype)


def token(row):
    return lax.rem(row, 4)


def expand(ml):
    col = jnp.transpose(jnp.broadcast_to(ml, (128, 128)))
    return col[0:64, :], col[64:128, :]


def compact(m, l):
    return jnp.transpose(jnp.concatenate([m, l], axis=0))[0:1, :]


def attend_kernel(chips, rows, scale, lens_ref, hid_ref, wq_ref, wr_ref, wk_ref, ckv_ref, kr_ref, out_ref,
                  wq_buf, wr_buf, wk_buf, wide, acc, lat_all, rope_all, s_buf, p_buf,
                  away_o, away_ml, home_o, home_ml, d2d_o, d2d_ml, one_o, one_ml, two_o, two_ml,
                  wq_sem, wr_sem, wk_sem, q_send, q_recv, send0, send1, send2, recv0, recv1, recv2):
    x, c, xr, xl, right, left, partner = place(chips)
    xo = lax.rem(x + 2, chips)
    i = pl.program_id(0)
    f32, bf16 = jnp.float32, jnp.bfloat16
    toks, dim = hid_ref.shape[1:]
    n = rows * toks
    pairs, nope = wq_ref.shape[1], wq_ref.shape[3]
    quarters = pairs // 2
    depth = dim // CUTS
    local_len, width = ckv_ref.shape[1:]
    gq = lat_all.shape[3]
    nq = chips * gq
    hq = gq // 2
    k2 = scale * LOG2E
    lanes = [pl.ds(j * 128, 128) for j in range(width // 128)]

    early = rows // 4
    top, low, every = pl.ds(0, early), pl.ds(early, rows - early), pl.ds(0, rows)
    pieces = [(lat_all, every, pl.ds(0, 16), 0), (lat_all, every, pl.ds(16, 16), 1)]
    for part, turn in ((top, 0), (low, 1)):
        pieces += [(lat_all, part, pl.ds(32, 16), 0), (lat_all, part, pl.ds(48, 16), 1),
                   (rope_all, part, pl.ds(0, hq), turn)]

    def give(p, kind, block, core, dev):
        array, part, queries, _ = pieces[p]
        ref = array.at[part, core, block, queries]
        return remote(ref, ref, q_send.at[p, kind], q_recv.at[p, kind], dev)

    def send_own(p):
        give(p, 0, x, c, right).start()
        give(p, 1, x, c, left).start()
        give(p, 2, x, c, partner).start()

    def second_hop(p):
        return give(p, 3, xr, c, left) if pieces[p][3] else give(p, 3, xl, c, right)

    def relay(p):
        give(p, 0, xl, c, partner).wait_recv()
        if pieces[p][3] == 0:
            second_hop(p).start()
        give(p, 4, xl, c, partner).start()
        give(p, 1, xr, c, partner).wait_recv()
        if pieces[p][3] == 1:
            second_hop(p).start()
        give(p, 5, xr, c, partner).start()

    def relay_far(p):
        give(p, 3, xo, c, partner).wait_recv()
        give(p, 6, xo, c, partner).start()

    def complete(p):
        for kind, block in ((2, x), (4, xl), (5, xr), (6, xo)):
            give(p, kind, block, 1 - c, partner).wait_recv()

    def sent(p):
        give(p, 0, x, c, right).wait_send()
        give(p, 1, x, c, left).wait_send()
        give(p, 2, x, c, partner).wait_send()
        second_hop(p).wait_send()
        give(p, 4, xl, c, partner).wait_send()
        give(p, 5, xr, c, partner).wait_send()
        give(p, 6, xo, c, partner).wait_send()

    def make_queries():
        barrier = pltpu.get_barrier_semaphore()
        for dev in (right, left, partner):
            pl.semaphore_signal(barrier, inc=1, device_id={"seq": dev}, device_id_type=MESH)

        def load(q, h, k):
            at = pl.ds(k * depth, depth)
            return pltpu.make_async_copy(wq_ref.at[at, 2 * q + h], wq_buf.at[h, at], wq_sem.at[h, k])

        def load_rope(half, j):
            return pltpu.make_async_copy(wr_ref.at[half * pairs + j], wr_buf.at[j % 4, half], wr_sem.at[half, j % 4])

        load_up = pltpu.make_async_copy(wk_ref, wk_buf, wk_sem)
        for k in range(CUTS):
            for h in range(2):
                load(0, h, k).start()
        load_up.start()
        for j in range(4):
            for half in range(2):
                load_rope(half, j).start()

        lane = lax.broadcasted_iota(jnp.int32, (128, 512), 1)
        src = lax.broadcasted_iota(jnp.int32, (128, 512), 0)
        spread = jnp.where(lax.rem(lane, 256) == 2 * src + lane // 256, 1.0, 0.0).astype(bf16)
        tiles = depth // 128
        for k in range(CUTS):
            stack = jnp.concatenate([hid_ref[:, :, (k * tiles + t) * 128:(k * tiles + t + 1) * 128].reshape(n, 128)
                                     for t in range(tiles)], axis=0)
            res = jnp.dot(stack, spread, preferred_element_type=f32).astype(bf16)
            for t in range(tiles):
                for side in range(2):
                    wide[k, pl.ds(side * n, n), pl.ds(t * 256, 256)] = res[t * n:(t + 1) * n,
                                                                           side * 256:side * 256 + 256]

        for q in range(quarters):
            acc[...] = jnp.zeros_like(acc)

            @pl.loop(0, CUTS // 2)
            def _(k):
                for h in range(2):
                    for e in range(2):
                        load(q, h, 2 * k + e).wait()
                for e in range(2):
                    w = [wq_buf.at[h, pl.ds((2 * k + e) * depth, depth)].reshape(2 * depth, nope)[...] for h in range(2)]
                    acc[e] += jnp.dot(wide[2 * k + e], jnp.concatenate(w, axis=1), preferred_element_type=f32)
                if q < quarters - 1:
                    for e in range(2):
                        for h in range(2):
                            load(q + 1, h, 2 * k + e).start()

            if q == 0:
                load_up.wait()
            q_lat = []
            for h in range(4):
                at = (pl.ds((h % 2) * n, n), pl.ds((h // 2) * nope, nope))
                q_n = (acc[0, *at] + acc[1, *at]).astype(bf16)
                q_lat.append(jnp.dot(q_n, wk_buf[4 * q + h], preferred_element_type=f32))
            pack(q_lat, lat_all.at[:, c, x], q * 16)
            if q == 0:
                pl.semaphore_wait(barrier, 3)
            send_own(q)
            if q == quarters - 1:
                relay(0)

        tokens = jnp.concatenate([hid_ref[:, :, t * 128:(t + 1) * 128].reshape(n, 128) for t in range(dim // 128)],
                                 axis=1)
        for q in range(2):
            q_rope = []
            for m in (2 * q, 2 * q + 1):
                for half in range(2):
                    load_rope(half, 2 * m).wait()
                    load_rope(half, 2 * m + 1).wait()
                w = wr_buf[pl.ds(2 * m % 4, 2)].reshape(256, dim)
                r = lax.dot_general(tokens, w, (((1,), (1,)), ((), ())), preferred_element_type=f32)
                if q == 0:
                    for half in range(2):
                        load_rope(half, 2 * m + 4).start()
                        load_rope(half, 2 * m + 5).start()
                q_rope += [r[:, 0:128], r[:, 128:256]]
            pack(q_rope, rope_all.at[:, c, x], 16 * q)
            if q == 0:
                relay(1)
        send_own(4)
        for p in range(2, 5):
            relay(p)
        for p in range(5, 8):
            send_own(p)
        for p in range(5):
            relay_far(p)
        for p in range(5):
            complete(p)

    def moves(r):
        a, h, d, e, t = (lax.rem(r, count) for count in (AWAY, HOME, PAIR, ONE, TWO))
        return (
            (away_o.at[a], d2d_o.at[d], partner),
            (away_ml.at[r], d2d_ml.at[r], partner),
            (home_o.at[h, xo, pl.ds(0, hq)], one_o.at[e, 0], right),
            (home_ml.at[r, xo], one_ml.at[r, 0], right),
            (home_o.at[h, xo, pl.ds(hq, hq)], one_o.at[e, 1], left),
            (home_ml.at[r, xo], one_ml.at[r, 1], left),
            (home_o.at[h, xr], two_o.at[t, 0], right),
            (home_ml.at[r, xr], two_ml.at[r, 0], right),
            (home_o.at[h, xl], two_o.at[t, 1], left),
            (home_ml.at[r, xl], two_ml.at[r, 1], left),
        )

    def copy(r, kind):
        src, dst, dev = moves(r)[kind]
        out, into, count, first = ((send0, recv0, PAIR, 0) if kind < 2 else (send1, recv1, ONE, 2) if kind < 6
                                   else (send2, recv2, TWO, 6))
        at = (lax.rem(r, count), kind - first)
        return remote(src, dst, out.at[at], into.at[at], dev)

    def late(lag):
        return jnp.where((i >= lag) & (i < rows + lag), i - lag, rows)

    def slot(r, count):
        return jnp.where(r < rows, lax.rem(r, count), count)

    def on_row(lag, act, kinds):
        @pl.when((i >= lag) & (i < rows + lag))
        def _():
            for kind in kinds:
                act(copy(i - lag, kind))

    def merge_pair():
        r = late(LAG_B)
        h, d = slot(r, HOME), slot(r, PAIR)
        for g in range(chips):
            ma, la = expand(home_ml[r, g])
            mb, lb = expand(d2d_ml[r, g])
            m = jnp.maximum(ma, mb)
            fa, fb = jnp.exp2((ma - m) * k2), jnp.exp2((mb - m) * k2)
            for at in lanes:
                home_o[h, g, :, at] = home_o[h, g, :, at] * fa + d2d_o[d, g, :, at] * fb
            home_ml[r, g] = compact(m, la * fa + lb * fb)

    def merge_half():
        r = late(LAG_C)
        h, e = slot(r, HOME), slot(r, ONE)
        for side, g in ((0, xr), (1, xl)):
            part = slice(side * hq, (side + 1) * hq)
            ma, la = expand(home_ml[r, g])
            mb, lb = expand(one_ml[r, side])
            m = jnp.maximum(ma, mb)[part]
            fa, fb = jnp.exp2((ma[part] - m) * k2), jnp.exp2((mb[part] - m) * k2)
            for at in lanes:
                home_o[h, g, pl.ds(side * hq, hq), at] = (home_o[h, g, pl.ds(side * hq, hq), at] * fa
                                                          + one_o[e, side, :, at] * fb)
            l = la[part] * fa + lb[part] * fb
            if side == 0:
                m, l = jnp.concatenate([m, ma[hq:]], axis=0), jnp.concatenate([l, la[hq:]], axis=0)
            else:
                m, l = jnp.concatenate([ma[:hq], m], axis=0), jnp.concatenate([la[:hq], l], axis=0)
            home_ml[r, g] = compact(m, l)

    def finish():
        r = late(LAG_D)
        h, e = slot(r, HOME), slot(r, TWO)
        ma, la = expand(home_ml[r, x])
        mb, lb = expand(two_ml[r, 0])
        mc, lc = expand(two_ml[r, 1])
        m = jnp.maximum(ma, jnp.maximum(mb, mc))
        fa, fb, fc = jnp.exp2((ma - m) * k2), jnp.exp2((mb - m) * k2), jnp.exp2((mc - m) * k2)
        l = la * fa + lb * fb + lc * fc
        for at in lanes:
            o = home_o[h, x, :, at] * fa + two_o[e, 0, :, at] * fb + two_o[e, 1, :, at] * fc
            out_ref[0, :, at] = (o / l).astype(out_ref.dtype)

    @pl.when(i == 0)
    def _():
        make_queries()

    @pl.when(i == early)
    def _():
        for p in range(5, 8):
            complete(p)

    on_row(AWAY, lambda cp: cp.wait_send(), range(0, 2))
    on_row(LAG_B + ONE, lambda cp: cp.wait_send(), range(2, 6))
    on_row(LAG_C + TWO, lambda cp: cp.wait_send(), range(6, 10))

    on_row(LAG_D, lambda cp: cp.wait_recv(), range(6, 10))

    @pl.when(i < rows)
    def _():
        base = (2 * x + c) * local_len
        row = jnp.minimum(i, rows - 1)
        seen = lens_ref[row] - base
        a, h = lax.rem(row, AWAY), lax.rem(row, HOME)
        col = lax.broadcasted_iota(jnp.int32, (nq, local_len), 1)
        tok = token(lax.broadcasted_iota(jnp.int32, (nq, 1), 0))
        visible = col <= seen + tok
        contract = (((1,), (1,)), ((), ()))

        def scores(k, block):
            lat = lat_all[row, block].reshape(nq, width)
            rope = jnp.concatenate([rope_all[row, block, g][:, e * 64:(e + 1) * 64] for g in range(chips) for e in range(2)],
                                   axis=0)
            s = lax.dot_general(lat, ckv_ref[0], contract, preferred_element_type=f32)
            s = s + jnp.dot(rope, kr_ref[0], preferred_element_type=f32)
            s_buf[k] = jnp.where(visible, s, MASK_FILL)

        def weigh(k):
            s = s_buf[k]
            m = jnp.max(s, axis=1, keepdims=True)
            p = jnp.exp2((s - m) * k2)
            l = jnp.sum(p, axis=1, keepdims=True)
            p_buf[k] = p.astype(bf16)
            return m, l

        def mix(k, m, l, o_ref, to, ml_ref):
            o = jnp.dot(p_buf[k], ckv_ref[0], preferred_element_type=f32)
            m = jnp.broadcast_to(m, (nq, 128))
            l = jnp.broadcast_to(l, (nq, 128))
            for g in range(chips):
                at = slice(g * gq, (g + 1) * gq)
                o_ref[to, g] = o[at]
                ml_ref[row, g] = compact(m[at], l[at])

        finish()
        scores(0, 1 - c)
        scores(1, c)
        on_row(LAG_B, lambda cp: cp.wait_recv(), range(0, 2))
        on_row(LAG_C, lambda cp: cp.wait_recv(), range(2, 6))
        merge_pair()
        merge_half()
        ml0 = weigh(0)
        mix(0, *ml0, away_o, a, away_ml)
        ml1 = weigh(1)
        mix(1, *ml1, home_o, h, home_ml)

    @pl.when(i >= rows)
    def _():
        on_row(LAG_B, lambda cp: cp.wait_recv(), range(0, 2))
        on_row(LAG_C, lambda cp: cp.wait_recv(), range(2, 6))
        merge_pair()
        merge_half()
        finish()

    on_row(0, lambda cp: cp.start(), range(0, 2))
    on_row(LAG_B, lambda cp: cp.start(), range(2, 6))
    on_row(LAG_C, lambda cp: cp.start(), range(6, 10))

    @pl.when(i == 0)
    def _():
        relay(5)

    @pl.when(i == 1)
    def _():
        relay(6)
        relay(7)

    @pl.when(i == 3)
    def _():
        for p in range(5, 8):
            relay_far(p)

    @pl.when(i == rows + LAG_D - 1)
    def _():
        for p in range(8):
            sent(p)

        for lag, kinds in ((LAG_B + ONE, range(2, 6)), (LAG_C + TWO, range(6, 10))):
            for r in range(rows + LAG_D - lag, rows):
                for kind in kinds:
                    copy(r, kind).wait_send()


def attend(chips, scale, lens, hidden, w_uq, w_qr, w_uk, ckv, kr):
    rows, toks, dim = hidden.shape
    heads, nope, width = w_uk.shape
    gq = heads * toks
    nq = chips * gq
    local_len = ckv.shape[1]
    wq = w_uq.reshape(dim, heads // 2, 2, nope)
    wr = jnp.transpose(w_qr, (1, 2, 0))
    row = lambda i: jnp.minimum(i, rows - 1)
    f32, bf16 = jnp.float32, jnp.bfloat16
    hbm = pl.BlockSpec(memory_space=pl.ANY)
    dma = pltpu.SemaphoreType.DMA
    return pl.pallas_call(
        functools.partial(attend_kernel, chips, rows, scale),
        grid=(rows + LAG_D,),
        out_shape=jax.ShapeDtypeStruct((rows, gq, width), bf16),
        in_specs=[pl.BlockSpec(memory_space=pltpu.SMEM), pl.BlockSpec(memory_space=pltpu.VMEM), hbm, hbm, hbm,
                  pl.BlockSpec((1,) + ckv.shape[1:], lambda i: (row(i), 0, 0)),
                  pl.BlockSpec((1,) + kr.shape[1:], lambda i: (row(i), 0, 0))],
        out_specs=pl.BlockSpec((1, gq, width), lambda i: (jnp.maximum(i - LAG_D, 0), 0, 0)),
        scratch_shapes=[
            pltpu.VMEM((2, dim, 2, nope), bf16), pltpu.VMEM((4, 2) + wr.shape[1:], bf16), pltpu.VMEM(w_uk.shape, bf16),
            pltpu.VMEM((CUTS, 2 * rows * toks, 2 * dim // CUTS), bf16), pltpu.VMEM((2, 2 * rows * toks, 2 * nope), f32),
            pltpu.VMEM((rows, 2, chips, gq, width), bf16), pltpu.VMEM((rows, 2, chips, gq // 2, 128), bf16),
            pltpu.VMEM((2, nq, local_len), f32), pltpu.VMEM((2, nq, local_len), bf16),
            pltpu.VMEM((AWAY, chips, gq, width), f32), pltpu.VMEM((rows + 1, chips, 1, 128), f32),
            pltpu.VMEM((HOME + 1, chips, gq, width), f32), pltpu.VMEM((rows + 1, chips, 1, 128), f32),
            pltpu.VMEM((PAIR + 1, chips, gq, width), f32), pltpu.VMEM((rows + 1, chips, 1, 128), f32),
            pltpu.VMEM((ONE + 1, 2, gq // 2, width), f32), pltpu.VMEM((rows + 1, 2, 1, 128), f32),
            pltpu.VMEM((TWO + 1, 2, gq, width), f32), pltpu.VMEM((rows + 1, 2, 1, 128), f32),
            dma((2, CUTS)), dma((2, 4)), dma(()), dma((8, 7)), dma((8, 7))]
            + 2 * [dma((PAIR, 2)), dma((ONE, 4)), dma((TWO, 4))],
        compiler_params=pltpu.CompilerParams(collective_id=1, has_side_effects=True,
                                             dimension_semantics=("arbitrary",), vmem_limit_bytes=67_000_000),
        name="attend_merge",
    )(lens, hidden, wq, wr, w_uk, ckv, kr)


def unpack(ref, slot):
    rows = ref.shape[0]
    tiles = [ref[b, pl.ds(slot, 16)].astype(jnp.float32) for b in range(rows)]
    vals = []
    for h in range(2):
        even = jnp.concatenate([t[8 * h:8 * h + 8] for t in tiles[0::2]], axis=0)
        odd = jnp.concatenate([t[8 * h:8 * h + 8] for t in tiles[1::2]], axis=0)
        n = even.shape[0]
        low = lax.rem(lax.broadcasted_iota(jnp.int32, even.shape, 0), 8) < 4
        vals += [jnp.where(low, even, pltpu.roll(odd, 4, 0)), jnp.where(low, pltpu.roll(even, n - 4, 0), odd)]
    return [v.astype(ref.dtype) for v in vals]


def output_kernel(chips, o_ref, hid_ref, wv_ref, w_ref, out_ref, o_buf, hid_buf, wv_buf, ov, w_buf,
                  away, near, home, one, two, in_sem, w_sem, send, recv):
    x, c, xr, xl, right, left, partner = place(chips)
    xo = lax.rem(x + 2, chips)
    cols = w_buf.shape[2]
    rows, toks = out_ref.shape[:2]
    span = lambda dev: pl.ds(pl.multiple_of(dev * cols, 128), cols)
    dests = (xo, xr, xl, x)
    order = []
    for k in range(chips):
        order += [2 * dests[k] + 1 - c, 2 * dests[k] + c]

    def load(n):
        return pltpu.make_async_copy(w_ref.at[:, span(order[n])], w_buf.at[n], w_sem.at[n])

    firsts = [pltpu.make_async_copy(o_ref, o_buf, in_sem.at[0]), pltpu.make_async_copy(wv_ref, wv_buf, in_sem.at[1]),
              pltpu.make_async_copy(hid_ref.at[:, :, span(2 * x + c)], hid_buf, in_sem.at[2])]
    for cp in firsts:
        cp.start()
    for n in range(AHEAD):
        load(n).start()
    greet((right, left, partner))

    firsts[0].wait()
    firsts[1].wait()
    value = wv_buf.shape[2]
    for q in range(wv_buf.shape[0] // 4):
        for h, o_lat in enumerate(unpack(o_buf, 16 * q)):
            ov[:, pl.ds((4 * q + h) * value, value)] = jnp.dot(
                o_lat, wv_buf[4 * q + h], preferred_element_type=jnp.float32).astype(ov.dtype)

    tokens = ov.shape[0]
    first, second = pl.ds(0, tokens // 2), pl.ds(tokens // 2, tokens // 2)

    def project(n):
        load(n).wait()
        if n + AHEAD < 2 * chips:
            load(n + AHEAD).start()
        return jnp.dot(ov[...], w_buf[n], preferred_element_type=jnp.float32)

    def swap(k):
        return remote(away.at[k], near.at[k], send.at[0, k], recv.at[0, k], partner)

    def hop(kind):
        src, dst, dev = ((home.at[0, first], one.at[0], right), (home.at[0, second], one.at[1], left),
                         (home.at[1, second], two.at[0, second], right), (home.at[2, first], two.at[1, first], left),
                         (home.at[1, first], two.at[0, first], right),
                         (home.at[2, second], two.at[1, second], left))[kind]
        return remote(src, dst, send.at[1, kind], recv.at[1, kind], dev)

    away[0] = project(0)
    swap(0).start()
    for k in range(chips):
        home[k] = project(2 * k + 1)
        swap(k).wait_recv()
        home[k] = home[k] + near[k]
        for kind in ((0, 1), (2,), (3,), ())[k]:
            hop(kind).start()
        if k + 1 < chips:
            away[k + 1] = project(2 * k + 2)
            swap(k + 1).start()
        if k == 1:
            hop(0).wait_recv()
            home[1, first] = home[1, first] + one[0]
            hop(4).start()
        if k == 2:
            hop(1).wait_recv()
            home[2, second] = home[2, second] + one[1]
            hop(5).start()
    firsts[2].wait()
    for kind in range(2, 6):
        hop(kind).wait_recv()
    y = home[chips - 1] + two[0] + two[1]
    out_ref[:, :, span(2 * x + c)] = (hid_buf[...].astype(jnp.float32) + y.reshape(rows, toks, cols)).astype(out_ref.dtype)

    whole, top, low = pl.ds(0, rows), pl.ds(0, rows // 2), pl.ds(rows // 2, rows // 2)

    def give(kind, part, block, core, dev):
        ref = out_ref.at[part, :, span(2 * block + core)]
        return remote(ref, ref, send.at[2, kind], recv.at[2, kind], dev)

    sends = [give(0, top, x, c, right), give(1, low, x, c, right), give(2, low, x, c, left), give(3, top, x, c, left),
             give(4, whole, x, c, partner), give(5, top, xl, c, right), give(6, low, xr, c, left),
             give(7, whole, xl, c, partner), give(8, whole, xr, c, partner),
             give(9, top, xo, c, partner), give(10, low, xo, c, partner)]
    for k in (0, 2, 1, 3, 4):
        sends[k].start()
    for kind, part, block, then in ((0, top, xl, 5), (2, low, xr, 6), (1, low, xl, 7), (3, top, xr, 8),
                                    (5, top, xo, 9), (6, low, xo, 10)):
        give(kind, part, block, c, partner).wait_recv()
        sends[then].start()
    for kind, part, block in ((4, whole, x), (7, whole, xl), (8, whole, xr), (9, top, xo), (10, low, xo)):
        give(kind, part, block, 1 - c, partner).wait_recv()
    for k in range(chips):
        swap(k).wait_send()
    for kind in range(6):
        hop(kind).wait_send()
    for cp in sends:
        cp.wait_send()


def output(chips, o_lat, hidden, w_uv, w_o):
    rows, toks, dim = hidden.shape
    tokens = rows * toks
    depth = w_o.shape[0]
    cols = dim // (2 * chips)
    f32 = jnp.float32
    vmem, hbm = pl.BlockSpec(memory_space=pltpu.VMEM), pl.BlockSpec(memory_space=pl.ANY)
    dma = pltpu.SemaphoreType.DMA
    return pl.pallas_call(
        functools.partial(output_kernel, chips),
        out_shape=jax.ShapeDtypeStruct(hidden.shape, hidden.dtype),
        in_specs=[hbm] * 4,
        out_specs=vmem,
        scratch_shapes=[
            pltpu.VMEM(o_lat.shape, o_lat.dtype), pltpu.VMEM((rows, toks, cols), hidden.dtype),
            pltpu.VMEM(w_uv.shape, w_uv.dtype), pltpu.VMEM((tokens, depth), o_lat.dtype),
            pltpu.VMEM((2 * chips, depth, cols), w_o.dtype),
            pltpu.VMEM((chips, tokens, cols), f32), pltpu.VMEM((chips, tokens, cols), f32),
            pltpu.VMEM((chips, tokens, cols), f32), pltpu.VMEM((2, tokens // 2, cols), f32),
            pltpu.VMEM((2, tokens, cols), f32),
            dma((3,)), dma((2 * chips,)), dma((3, 11)), dma((3, 11))],
        compiler_params=pltpu.CompilerParams(collective_id=2, has_side_effects=True, vmem_limit_bytes=65_500_000),
        name="project_output",
    )(o_lat, hidden, w_uv, w_o)


def solution(mesh):
    chips = mesh.shape["seq"] // 2

    def local_step(hidden, cache_lens, c_kv, k_r, w_uq, w_qr, w_uk, w_uv, w_o):
        rows, toks, dim = hidden.shape
        heads, nope, width = w_uk.shape
        rope_dim = w_qr.shape[2]
        value = w_uv.shape[2]
        score_scale = (nope + rope_dim) ** -0.5
        o_lat = attend(chips, score_scale, cache_lens, hidden, w_uq, w_qr, w_uk, c_kv, jnp.swapaxes(k_r, 1, 2))
        return output(chips, o_lat, hidden, w_uv, w_o.reshape(heads * value, dim))

    specs_in = (P("batch", None, None), P("batch"), P("batch", "seq", None), P("batch", "seq", None),
                P(None, "seq", None), P(None, "seq", None), P("seq", None, None), P("seq", None, None),
                P("seq", None, None))
    return jax.shard_map(local_step, mesh=mesh, in_specs=specs_in, out_specs=P("batch", None, None), check_vma=False)
```

```python
import functools

import jax
import jax.numpy as jnp
from jax import lax
from jax.experimental import pallas as pl
from jax.experimental.pallas import tpu as pltpu
from jax.sharding import PartitionSpec as P

MASK_FILL = -1e30
LOG2E = 1.4426950408889634
MESH = pl.DeviceIdType.MESH
LAG_B, LAG_C, LAG_D = 1, 3, 6
CUTS = 4
AHEAD = 3
AWAY, HOME, PAIR, ONE, TWO = 4, 10, 4, 4, 6


def remote(src, dst, send_sem, recv_sem, dev):
    return pltpu.make_async_remote_copy(src_ref=src, dst_ref=dst, send_sem=send_sem, recv_sem=recv_sem,
                                        device_id={"seq": dev}, device_id_type=MESH)


def place(chips):
    me = lax.axis_index("seq")
    x, c = me // 2, lax.rem(me, 2)
    xr, xl = lax.rem(x + 1, chips), lax.rem(x + chips - 1, chips)
    return x, c, xr, xl, 2 * xr + c, 2 * xl + c, 2 * x + 1 - c


def greet(devs):
    barrier = pltpu.get_barrier_semaphore()
    for dev in devs:
        pl.semaphore_signal(barrier, inc=1, device_id={"seq": dev}, device_id_type=MESH)
    pl.semaphore_wait(barrier, len(devs))


def pack(vals, dst, slot):
    n = vals[0].shape[0]
    low = lax.rem(lax.broadcasted_iota(jnp.int32, vals[0].shape, 0), 8) < 4
    even = [jnp.where(low, p, pltpu.roll(q, 4, 0)) for p, q in (vals[:2], vals[2:])]
    odd = [jnp.where(low, pltpu.roll(p, n - 4, 0), q) for p, q in (vals[:2], vals[2:])]
    for v in range(n // 8):
        at = slice(8 * v, 8 * v + 8)
        for side, both in ((0, even), (1, odd)):
            dst[2 * v + side, pl.ds(slot, 16)] = jnp.concatenate([both[0][at], both[1][at]], axis=0).astype(dst.dtype)


def token(row):
    return lax.rem(row, 4)


def expand(ml):
    col = jnp.transpose(jnp.broadcast_to(ml, (128, 128)))
    return col[0:64, :], col[64:128, :]


def compact(m, l):
    return jnp.transpose(jnp.concatenate([m, l], axis=0))[0:1, :]


def attend_kernel(chips, rows, scale, lens_ref, hid_ref, wq_ref, wr_ref, wk_ref, ckv_ref, kr_ref, out_ref,
                  wq_buf, wr_buf, wk_buf, wide, acc, lat_all, rope_all, s_buf, p_buf,
                  away_o, away_ml, home_o, home_ml, d2d_o, d2d_ml, one_o, one_ml, two_o, two_ml,
                  wq_sem, wr_sem, wk_sem, q_send, q_recv, send0, send1, send2, recv0, recv1, recv2):
    x, c, xr, xl, right, left, partner = place(chips)
    xo = lax.rem(x + 2, chips)
    i = pl.program_id(0)
    f32, bf16 = jnp.float32, jnp.bfloat16
    toks, dim = hid_ref.shape[1:]
    n = rows * toks
    pairs, nope = wq_ref.shape[1], wq_ref.shape[3]
    quarters = pairs // 2
    depth = dim // CUTS
    local_len, width = ckv_ref.shape[1:]
    gq = lat_all.shape[3]
    nq = chips * gq
    hq = gq // 2
    k2 = scale * LOG2E
    lanes = [pl.ds(j * 128, 128) for j in range(width // 128)]

    early = rows // 4
    top, low, every = pl.ds(0, early), pl.ds(early, rows - early), pl.ds(0, rows)
    pieces = [(lat_all, every, pl.ds(0, 16), 0), (lat_all, every, pl.ds(16, 16), 1)]
    for part, turn in ((top, 0), (low, 1)):
        pieces += [(lat_all, part, pl.ds(32, 16), 0), (lat_all, part, pl.ds(48, 16), 1),
                   (rope_all, part, pl.ds(0, hq), turn)]

    def give(p, kind, block, core, dev):
        array, part, queries, _ = pieces[p]
        ref = array.at[part, core, block, queries]
        return remote(ref, ref, q_send.at[p, kind], q_recv.at[p, kind], dev)

    def send_own(p):
        give(p, 0, x, c, right).start()
        give(p, 1, x, c, left).start()
        give(p, 2, x, c, partner).start()

    def second_hop(p):
        return give(p, 3, xr, c, left) if pieces[p][3] else give(p, 3, xl, c, right)

    def relay(p):
        give(p, 0, xl, c, partner).wait_recv()
        if pieces[p][3] == 0:
            second_hop(p).start()
        give(p, 4, xl, c, partner).start()
        give(p, 1, xr, c, partner).wait_recv()
        if pieces[p][3] == 1:
            second_hop(p).start()
        give(p, 5, xr, c, partner).start()

    def relay_far(p):
        give(p, 3, xo, c, partner).wait_recv()
        give(p, 6, xo, c, partner).start()

    def complete(p):
        for kind, block in ((2, x), (4, xl), (5, xr), (6, xo)):
            give(p, kind, block, 1 - c, partner).wait_recv()

    def sent(p):
        give(p, 0, x, c, right).wait_send()
        give(p, 1, x, c, left).wait_send()
        give(p, 2, x, c, partner).wait_send()
        second_hop(p).wait_send()
        give(p, 4, xl, c, partner).wait_send()
        give(p, 5, xr, c, partner).wait_send()
        give(p, 6, xo, c, partner).wait_send()

    def make_queries():
        barrier = pltpu.get_barrier_semaphore()
        for dev in (right, left, partner):
            pl.semaphore_signal(barrier, inc=1, device_id={"seq": dev}, device_id_type=MESH)

        def load(q, h, k):
            at = pl.ds(k * depth, depth)
            return pltpu.make_async_copy(wq_ref.at[at, 2 * q + h], wq_buf.at[h, at], wq_sem.at[h, k])

        def load_rope(half, j):
            return pltpu.make_async_copy(wr_ref.at[half * pairs + j], wr_buf.at[j % 4, half], wr_sem.at[half, j % 4])

        load_up = pltpu.make_async_copy(wk_ref, wk_buf, wk_sem)
        for k in range(CUTS):
            for h in range(2):
                load(0, h, k).start()
        load_up.start()

        lane = lax.broadcasted_iota(jnp.int32, (128, 512), 1)
        src = lax.broadcasted_iota(jnp.int32, (128, 512), 0)
        spread = jnp.where(lax.rem(lane, 256) == 2 * src + lane // 256, 1.0, 0.0).astype(bf16)
        tiles = depth // 128
        for k in range(CUTS):
            stack = jnp.concatenate([hid_ref[:, :, (k * tiles + t) * 128:(k * tiles + t + 1) * 128].reshape(n, 128)
                                     for t in range(tiles)], axis=0)
            res = jnp.dot(stack, spread, preferred_element_type=f32).astype(bf16)
            for t in range(tiles):
                for side in range(2):
                    wide[k, pl.ds(side * n, n), pl.ds(t * 256, 256)] = res[t * n:(t + 1) * n,
                                                                           side * 256:side * 256 + 256]

        for q in range(quarters):
            acc[...] = jnp.zeros_like(acc)

            @pl.loop(0, CUTS // 2)
            def _(k):
                for h in range(2):
                    for e in range(2):
                        load(q, h, 2 * k + e).wait()
                for e in range(2):
                    w = [wq_buf.at[h, pl.ds((2 * k + e) * depth, depth)].reshape(2 * depth, nope)[...] for h in range(2)]
                    acc[e] += jnp.dot(wide[2 * k + e], jnp.concatenate(w, axis=1), preferred_element_type=f32)
                if q < quarters - 1:
                    for e in range(2):
                        for h in range(2):
                            load(q + 1, h, 2 * k + e).start()

            if q == 0:
                load_up.wait()
            q_lat = []
            for h in range(4):
                at = (pl.ds((h % 2) * n, n), pl.ds((h // 2) * nope, nope))
                q_n = (acc[0, *at] + acc[1, *at]).astype(bf16)
                q_lat.append(jnp.dot(q_n, wk_buf[4 * q + h], preferred_element_type=f32))
            pack(q_lat, lat_all.at[:, c, x], q * 16)
            if q == 0:
                pl.semaphore_wait(barrier, 3)
            send_own(q)
            if q == quarters - 3:
                for j in range(4):
                    for half in range(2):
                        load_rope(half, j).start()
            if q == quarters - 1:
                relay(0)

        tokens = jnp.concatenate([hid_ref[:, :, t * 128:(t + 1) * 128].reshape(n, 128) for t in range(dim // 128)],
                                 axis=1)
        for q in range(2):
            q_rope = []
            for m in (2 * q, 2 * q + 1):
                for half in range(2):
                    load_rope(half, 2 * m).wait()
                    load_rope(half, 2 * m + 1).wait()
                w = wr_buf[pl.ds(2 * m % 4, 2)].reshape(256, dim)
                r = lax.dot_general(tokens, w, (((1,), (1,)), ((), ())), preferred_element_type=f32)
                if q == 0:
                    for half in range(2):
                        load_rope(half, 2 * m + 4).start()
                        load_rope(half, 2 * m + 5).start()
                q_rope += [r[:, 0:128], r[:, 128:256]]
            pack(q_rope, rope_all.at[:, c, x], 16 * q)
            if q == 0:
                relay(1)
        send_own(4)
        for p in range(2, 5):
            relay(p)
        for p in range(5, 8):
            send_own(p)
        for p in range(5):
            relay_far(p)
        for p in range(5):
            complete(p)

    def moves(r):
        a, h, d, e, t = (lax.rem(r, count) for count in (AWAY, HOME, PAIR, ONE, TWO))
        return (
            (away_o.at[a], d2d_o.at[d], partner),
            (away_ml.at[r], d2d_ml.at[r], partner),
            (home_o.at[h, xo, pl.ds(0, hq)], one_o.at[e, 0], right),
            (home_ml.at[r, xo], one_ml.at[r, 0], right),
            (home_o.at[h, xo, pl.ds(hq, hq)], one_o.at[e, 1], left),
            (home_ml.at[r, xo], one_ml.at[r, 1], left),
            (home_o.at[h, xr], two_o.at[t, 0], right),
            (home_ml.at[r, xr], two_ml.at[r, 0], right),
            (home_o.at[h, xl], two_o.at[t, 1], left),
            (home_ml.at[r, xl], two_ml.at[r, 1], left),
        )

    def copy(r, kind):
        src, dst, dev = moves(r)[kind]
        out, into, count, first = ((send0, recv0, PAIR, 0) if kind < 2 else (send1, recv1, ONE, 2) if kind < 6
                                   else (send2, recv2, TWO, 6))
        at = (lax.rem(r, count), kind - first)
        return remote(src, dst, out.at[at], into.at[at], dev)

    def late(lag):
        return jnp.where((i >= lag) & (i < rows + lag), i - lag, rows)

    def slot(r, count):
        return jnp.where(r < rows, lax.rem(r, count), count)

    def on_row(lag, act, kinds):
        @pl.when((i >= lag) & (i < rows + lag))
        def _():
            for kind in kinds:
                act(copy(i - lag, kind))

    def merge_pair():
        r = late(LAG_B)
        h, d = slot(r, HOME), slot(r, PAIR)
        for g in range(chips):
            ma, la = expand(home_ml[r, g])
            mb, lb = expand(d2d_ml[r, g])
            m = jnp.maximum(ma, mb)
            fa, fb = jnp.exp2((ma - m) * k2), jnp.exp2((mb - m) * k2)
            for at in lanes:
                home_o[h, g, :, at] = home_o[h, g, :, at] * fa + d2d_o[d, g, :, at] * fb
            home_ml[r, g] = compact(m, la * fa + lb * fb)

    def merge_half():
        r = late(LAG_C)
        h, e = slot(r, HOME), slot(r, ONE)
        for side, g in ((0, xr), (1, xl)):
            part = slice(side * hq, (side + 1) * hq)
            ma, la = expand(home_ml[r, g])
            mb, lb = expand(one_ml[r, side])
            m = jnp.maximum(ma, mb)[part]
            fa, fb = jnp.exp2((ma[part] - m) * k2), jnp.exp2((mb[part] - m) * k2)
            for at in lanes:
                home_o[h, g, pl.ds(side * hq, hq), at] = (home_o[h, g, pl.ds(side * hq, hq), at] * fa
                                                          + one_o[e, side, :, at] * fb)
            l = la[part] * fa + lb[part] * fb
            if side == 0:
                m, l = jnp.concatenate([m, ma[hq:]], axis=0), jnp.concatenate([l, la[hq:]], axis=0)
            else:
                m, l = jnp.concatenate([ma[:hq], m], axis=0), jnp.concatenate([la[:hq], l], axis=0)
            home_ml[r, g] = compact(m, l)

    def finish():
        r = late(LAG_D)
        h, e = slot(r, HOME), slot(r, TWO)
        ma, la = expand(home_ml[r, x])
        mb, lb = expand(two_ml[r, 0])
        mc, lc = expand(two_ml[r, 1])
        m = jnp.maximum(ma, jnp.maximum(mb, mc))
        fa, fb, fc = jnp.exp2((ma - m) * k2), jnp.exp2((mb - m) * k2), jnp.exp2((mc - m) * k2)
        l = la * fa + lb * fb + lc * fc
        for at in lanes:
            o = home_o[h, x, :, at] * fa + two_o[e, 0, :, at] * fb + two_o[e, 1, :, at] * fc
            out_ref[0, :, at] = (o / l).astype(out_ref.dtype)

    @pl.when(i == 0)
    def _():
        make_queries()

    @pl.when(i == early)
    def _():
        for p in range(5, 8):
            complete(p)

    on_row(AWAY, lambda cp: cp.wait_send(), range(0, 2))
    on_row(LAG_B + ONE, lambda cp: cp.wait_send(), range(2, 6))
    on_row(LAG_C + TWO, lambda cp: cp.wait_send(), range(6, 10))

    on_row(LAG_D, lambda cp: cp.wait_recv(), range(6, 10))

    @pl.when(i < rows)
    def _():
        base = (2 * x + c) * local_len
        row = jnp.minimum(i, rows - 1)
        seen = lens_ref[row] - base
        a, h = lax.rem(row, AWAY), lax.rem(row, HOME)
        col = lax.broadcasted_iota(jnp.int32, (nq, local_len), 1)
        tok = token(lax.broadcasted_iota(jnp.int32, (nq, 1), 0))
        visible = col <= seen + tok
        contract = (((1,), (1,)), ((), ()))

        def scores(k, block):
            lat = lat_all[row, block].reshape(nq, width)
            rope = jnp.concatenate([rope_all[row, block, g][:, e * 64:(e + 1) * 64] for g in range(chips) for e in range(2)],
                                   axis=0)
            s = lax.dot_general(lat, ckv_ref[0], contract, preferred_element_type=f32)
            s = s + jnp.dot(rope, kr_ref[0], preferred_element_type=f32)
            s_buf[k] = jnp.where(visible, s, MASK_FILL)

        def weigh(k):
            s = s_buf[k]
            m = jnp.max(s, axis=1, keepdims=True)
            p = jnp.exp2((s - m) * k2)
            l = jnp.sum(p, axis=1, keepdims=True)
            p_buf[k] = p.astype(bf16)
            return m, l

        def mix(k, m, l, o_ref, to, ml_ref):
            o = jnp.dot(p_buf[k], ckv_ref[0], preferred_element_type=f32)
            m = jnp.broadcast_to(m, (nq, 128))
            l = jnp.broadcast_to(l, (nq, 128))
            for g in range(chips):
                at = slice(g * gq, (g + 1) * gq)
                o_ref[to, g] = o[at]
                ml_ref[row, g] = compact(m[at], l[at])

        finish()
        scores(0, 1 - c)
        scores(1, c)
        on_row(LAG_B, lambda cp: cp.wait_recv(), range(0, 2))
        on_row(LAG_C, lambda cp: cp.wait_recv(), range(2, 6))
        merge_pair()
        merge_half()
        ml0 = weigh(0)
        mix(0, *ml0, away_o, a, away_ml)
        ml1 = weigh(1)
        mix(1, *ml1, home_o, h, home_ml)

    @pl.when(i >= rows)
    def _():
        on_row(LAG_B, lambda cp: cp.wait_recv(), range(0, 2))
        on_row(LAG_C, lambda cp: cp.wait_recv(), range(2, 6))
        merge_pair()
        merge_half()
        finish()

    on_row(0, lambda cp: cp.start(), range(0, 2))
    on_row(LAG_B, lambda cp: cp.start(), range(2, 6))
    on_row(LAG_C, lambda cp: cp.start(), range(6, 10))

    @pl.when(i == 0)
    def _():
        relay(5)

    @pl.when(i == 1)
    def _():
        relay(6)
        relay(7)

    @pl.when(i == 3)
    def _():
        for p in range(5, 8):
            relay_far(p)

    @pl.when(i == rows + LAG_D - 1)
    def _():
        for p in range(8):
            sent(p)

        for lag, kinds in ((LAG_B + ONE, range(2, 6)), (LAG_C + TWO, range(6, 10))):
            for r in range(rows + LAG_D - lag, rows):
                for kind in kinds:
                    copy(r, kind).wait_send()


def attend(chips, scale, lens, hidden, w_uq, w_qr, w_uk, ckv, kr):
    rows, toks, dim = hidden.shape
    heads, nope, width = w_uk.shape
    gq = heads * toks
    nq = chips * gq
    local_len = ckv.shape[1]
    wq = w_uq.reshape(dim, heads // 2, 2, nope)
    wr = jnp.transpose(w_qr, (1, 2, 0))
    row = lambda i: jnp.minimum(i, rows - 1)
    f32, bf16 = jnp.float32, jnp.bfloat16
    hbm = pl.BlockSpec(memory_space=pl.ANY)
    dma = pltpu.SemaphoreType.DMA
    return pl.pallas_call(
        functools.partial(attend_kernel, chips, rows, scale),
        grid=(rows + LAG_D,),
        out_shape=jax.ShapeDtypeStruct((rows, gq, width), bf16),
        in_specs=[pl.BlockSpec(memory_space=pltpu.SMEM), pl.BlockSpec(memory_space=pltpu.VMEM), hbm, hbm, hbm,
                  pl.BlockSpec((1,) + ckv.shape[1:], lambda i: (row(i), 0, 0)),
                  pl.BlockSpec((1,) + kr.shape[1:], lambda i: (row(i), 0, 0))],
        out_specs=pl.BlockSpec((1, gq, width), lambda i: (jnp.maximum(i - LAG_D, 0), 0, 0)),
        scratch_shapes=[
            pltpu.VMEM((2, dim, 2, nope), bf16), pltpu.VMEM((4, 2) + wr.shape[1:], bf16), pltpu.VMEM(w_uk.shape, bf16),
            pltpu.VMEM((CUTS, 2 * rows * toks, 2 * dim // CUTS), bf16), pltpu.VMEM((2, 2 * rows * toks, 2 * nope), f32),
            pltpu.VMEM((rows, 2, chips, gq, width), bf16), pltpu.VMEM((rows, 2, chips, gq // 2, 128), bf16),
            pltpu.VMEM((2, nq, local_len), f32), pltpu.VMEM((2, nq, local_len), bf16),
            pltpu.VMEM((AWAY, chips, gq, width), f32), pltpu.VMEM((rows + 1, chips, 1, 128), f32),
            pltpu.VMEM((HOME + 1, chips, gq, width), f32), pltpu.VMEM((rows + 1, chips, 1, 128), f32),
            pltpu.VMEM((PAIR + 1, chips, gq, width), f32), pltpu.VMEM((rows + 1, chips, 1, 128), f32),
            pltpu.VMEM((ONE + 1, 2, gq // 2, width), f32), pltpu.VMEM((rows + 1, 2, 1, 128), f32),
            pltpu.VMEM((TWO + 1, 2, gq, width), f32), pltpu.VMEM((rows + 1, 2, 1, 128), f32),
            dma((2, CUTS)), dma((2, 4)), dma(()), dma((8, 7)), dma((8, 7))]
            + 2 * [dma((PAIR, 2)), dma((ONE, 4)), dma((TWO, 4))],
        compiler_params=pltpu.CompilerParams(collective_id=1, has_side_effects=True,
                                             dimension_semantics=("arbitrary",), vmem_limit_bytes=67_000_000),
        name="attend_merge",
    )(lens, hidden, wq, wr, w_uk, ckv, kr)


def unpack(ref, slot):
    rows = ref.shape[0]
    tiles = [ref[b, pl.ds(slot, 16)].astype(jnp.float32) for b in range(rows)]
    vals = []
    for h in range(2):
        even = jnp.concatenate([t[8 * h:8 * h + 8] for t in tiles[0::2]], axis=0)
        odd = jnp.concatenate([t[8 * h:8 * h + 8] for t in tiles[1::2]], axis=0)
        n = even.shape[0]
        low = lax.rem(lax.broadcasted_iota(jnp.int32, even.shape, 0), 8) < 4
        vals += [jnp.where(low, even, pltpu.roll(odd, 4, 0)), jnp.where(low, pltpu.roll(even, n - 4, 0), odd)]
    return [v.astype(ref.dtype) for v in vals]


def output_kernel(chips, o_ref, hid_ref, wv_ref, w_ref, out_ref, o_buf, hid_buf, wv_buf, ov, w_buf,
                  away, near, home, one, two, in_sem, w_sem, send, recv):
    x, c, xr, xl, right, left, partner = place(chips)
    xo = lax.rem(x + 2, chips)
    cols = w_buf.shape[2]
    rows, toks = out_ref.shape[:2]
    span = lambda dev: pl.ds(pl.multiple_of(dev * cols, 128), cols)
    dests = (xo, xr, xl, x)
    order = []
    for k in range(chips):
        order += [2 * dests[k] + 1 - c, 2 * dests[k] + c]

    def load(n):
        return pltpu.make_async_copy(w_ref.at[:, span(order[n])], w_buf.at[n], w_sem.at[n])

    firsts = [pltpu.make_async_copy(o_ref, o_buf, in_sem.at[0]), pltpu.make_async_copy(wv_ref, wv_buf, in_sem.at[1]),
              pltpu.make_async_copy(hid_ref.at[:, :, span(2 * x + c)], hid_buf, in_sem.at[2])]
    for cp in firsts:
        cp.start()
    for n in range(AHEAD):
        load(n).start()
    greet((right, left, partner))

    firsts[0].wait()
    firsts[1].wait()
    value = wv_buf.shape[2]
    for q in range(wv_buf.shape[0] // 4):
        for h, o_lat in enumerate(unpack(o_buf, 16 * q)):
            ov[:, pl.ds((4 * q + h) * value, value)] = jnp.dot(
                o_lat, wv_buf[4 * q + h], preferred_element_type=jnp.float32).astype(ov.dtype)

    tokens = ov.shape[0]
    first, second = pl.ds(0, tokens // 2), pl.ds(tokens // 2, tokens // 2)

    def project(n):
        load(n).wait()
        if n + AHEAD < 2 * chips:
            load(n + AHEAD).start()
        return jnp.dot(ov[...], w_buf[n], preferred_element_type=jnp.float32)

    def swap(k):
        return remote(away.at[k], near.at[k], send.at[0, k], recv.at[0, k], partner)

    def hop(kind):
        src, dst, dev = ((home.at[0, first], one.at[0], right), (home.at[0, second], one.at[1], left),
                         (home.at[1, second], two.at[0, second], right), (home.at[2, first], two.at[1, first], left),
                         (home.at[1, first], two.at[0, first], right),
                         (home.at[2, second], two.at[1, second], left))[kind]
        return remote(src, dst, send.at[1, kind], recv.at[1, kind], dev)

    away[0] = project(0)
    swap(0).start()
    for k in range(chips):
        home[k] = project(2 * k + 1)
        swap(k).wait_recv()
        home[k] = home[k] + near[k]
        for kind in ((0, 1), (2,), (3,), ())[k]:
            hop(kind).start()
        if k + 1 < chips:
            away[k + 1] = project(2 * k + 2)
            swap(k + 1).start()
        if k == 1:
            hop(0).wait_recv()
            home[1, first] = home[1, first] + one[0]
            hop(4).start()
        if k == 2:
            hop(1).wait_recv()
            home[2, second] = home[2, second] + one[1]
            hop(5).start()
    firsts[2].wait()
    for kind in range(2, 6):
        hop(kind).wait_recv()
    y = home[chips - 1] + two[0] + two[1]
    out_ref[:, :, span(2 * x + c)] = (hid_buf[...].astype(jnp.float32) + y.reshape(rows, toks, cols)).astype(out_ref.dtype)

    whole, top, low = pl.ds(0, rows), pl.ds(0, rows // 2), pl.ds(rows // 2, rows // 2)

    def give(kind, part, block, core, dev):
        ref = out_ref.at[part, :, span(2 * block + core)]
        return remote(ref, ref, send.at[2, kind], recv.at[2, kind], dev)

    sends = [give(0, top, x, c, right), give(1, low, x, c, right), give(2, low, x, c, left), give(3, top, x, c, left),
             give(4, whole, x, c, partner), give(5, top, xl, c, right), give(6, low, xr, c, left),
             give(7, whole, xl, c, partner), give(8, whole, xr, c, partner),
             give(9, top, xo, c, partner), give(10, low, xo, c, partner)]
    for k in (0, 2, 1, 3, 4):
        sends[k].start()
    for kind, part, block, then in ((0, top, xl, 5), (2, low, xr, 6), (1, low, xl, 7), (3, top, xr, 8),
                                    (5, top, xo, 9), (6, low, xo, 10)):
        give(kind, part, block, c, partner).wait_recv()
        sends[then].start()
    for kind, part, block in ((4, whole, x), (7, whole, xl), (8, whole, xr), (9, top, xo), (10, low, xo)):
        give(kind, part, block, 1 - c, partner).wait_recv()
    for k in range(chips):
        swap(k).wait_send()
    for kind in range(6):
        hop(kind).wait_send()
    for cp in sends:
        cp.wait_send()


def output(chips, o_lat, hidden, w_uv, w_o):
    rows, toks, dim = hidden.shape
    tokens = rows * toks
    depth = w_o.shape[0]
    cols = dim // (2 * chips)
    f32 = jnp.float32
    vmem, hbm = pl.BlockSpec(memory_space=pltpu.VMEM), pl.BlockSpec(memory_space=pl.ANY)
    dma = pltpu.SemaphoreType.DMA
    return pl.pallas_call(
        functools.partial(output_kernel, chips),
        out_shape=jax.ShapeDtypeStruct(hidden.shape, hidden.dtype),
        in_specs=[hbm] * 4,
        out_specs=vmem,
        scratch_shapes=[
            pltpu.VMEM(o_lat.shape, o_lat.dtype), pltpu.VMEM((rows, toks, cols), hidden.dtype),
            pltpu.VMEM(w_uv.shape, w_uv.dtype), pltpu.VMEM((tokens, depth), o_lat.dtype),
            pltpu.VMEM((2 * chips, depth, cols), w_o.dtype),
            pltpu.VMEM((chips, tokens, cols), f32), pltpu.VMEM((chips, tokens, cols), f32),
            pltpu.VMEM((chips, tokens, cols), f32), pltpu.VMEM((2, tokens // 2, cols), f32),
            pltpu.VMEM((2, tokens, cols), f32),
            dma((3,)), dma((2 * chips,)), dma((3, 11)), dma((3, 11))],
        compiler_params=pltpu.CompilerParams(collective_id=2, has_side_effects=True, vmem_limit_bytes=55_000_000),
        name="project_output",
    )(o_lat, hidden, w_uv, w_o)


def solution(mesh):
    chips = mesh.shape["seq"] // 2

    def local_step(hidden, cache_lens, c_kv, k_r, w_uq, w_qr, w_uk, w_uv, w_o):
        rows, toks, dim = hidden.shape
        heads, nope, width = w_uk.shape
        rope_dim = w_qr.shape[2]
        value = w_uv.shape[2]
        score_scale = (nope + rope_dim) ** -0.5
        o_lat = attend(chips, score_scale, cache_lens, hidden, w_uq, w_qr, w_uk, c_kv, jnp.swapaxes(k_r, 1, 2))
        return output(chips, o_lat, hidden, w_uv, w_o.reshape(heads * value, dim))

    specs_in = (P("batch", None, None), P("batch"), P("batch", "seq", None), P("batch", "seq", None),
                P(None, "seq", None), P(None, "seq", None), P("seq", None, None), P("seq", None, None),
                P("seq", None, None))
    return jax.shard_map(local_step, mesh=mesh, in_specs=specs_in, out_specs=P("batch", None, None), check_vma=False)
```
